32 devices in a mesh: rep: 2 (over x), kv: 16 (over z, y, core).
Axes of the slice: x: 2, y: 2, z: 4, core: 2. Of those that a mesh axis runs over, the one named last changes fastest.
Arguments:
- queries: bfloat16 [32, 3, 36864], P('rep', None, 'kv'), parts along dimension 0, may hold values from -4 to 4
- cache: bfloat16 [8192, 16, 576], P(('rep', 'kv')), parts along dimension 0, may hold values from -4 to 4
- page_counts: int32 [32], P('rep'), parts along dimension 0, may hold values from 1 to 2048, as said below
- slot_request: int32 [1024], P(('rep', 'kv')), parts along dimension 0, may hold values from 0 to 15, as said below
- slot_start: int32 [1024], P(('rep', 'kv')), parts along dimension 0, may hold values from 0 to 2040, as said below
- slot_live: int32 [1024], P(('rep', 'kv')), parts along dimension 0, may hold values from 1 to 8, as said below
- slot_pages: int32 [1024, 8], P(('rep', 'kv')), parts along dimension 0, may hold values from 0 to 255, as said below
Outputs:
- attended: bfloat16 [32, 3, 32768], P('rep', None, 'kv'), parts along dimension 0
- lse: float32 [32, 3, 64], P('rep'), parts along dimension 0
The draws below stay inside these ranges and needn't reach their ends.
There are 2 independent parts, one for each index of `rep`. The reference program is written for one: setup_inputs(seed, part) draws one part's arguments, and reference() takes and returns one part's arrays. A program takes and returns all parts, laid end to end along the dimension named above; each array names one. Nothing has to cross between parts.
Inputs may be any that keep to these rules, and one draw needn't show every extreme that they name: Request r has 16 * page_counts[r] tokens; the slots that name r cover its pages 0 to page_counts[r] - 1, each exactly once; one request holds 8 * (256) pages. `slot_request`: every request is named by at least one slot; slot s lives on index s // 32 of kv. Slot s covers pages slot_start[s] to slot_start[s] + slot_live[s] - 1 of its request. Only the first slot_live[s] entries of slot_pages[s] are used. `slot_pages`: page numbers local to the device that holds the slot; all entries of one device's slots are distinct.
All inputs are finite; a program needn't handle non-finite values.
Results may differ from the reference program's by a relative error of at most 0.0043.
Values may be sent and summed in bfloat16 or wider, within the bound.
A program may use at most 128 MiB of HBM per device.

```python
import jax
import jax.numpy as jnp
import numpy as np
from jax import lax

H = 64
LAT = 512
ROPE = 64
PAGE = 16
SPAN = 8
QN = 3
REQS = 16
ITEMS = 32
P_DEV = 256
SLOTS = 512
PAGES = 4096


def plan_tables(key):
    heavy = SLOTS // 2
    weights = np.array([720720 // ((position + 2) * (position + 2)) for position in range(REQS - 1)], dtype=np.int64)
    spare = SLOTS - heavy - (REQS - 1)
    rest = spare * weights // weights.sum() + 1
    rest[0] += SLOTS - heavy - rest.sum()
    shares = np.concatenate([np.array([heavy], dtype=np.int64), rest])
    bounds = np.cumsum(shares)
    firsts = bounds - shares
    rank_at = np.searchsorted(bounds, np.arange(SLOTS), side='right').astype(np.int32)
    base_key = jax.random.fold_in(key, 1234)
    order_key, request_key, live_key, page_key = jax.random.split(base_key, 4)
    order = jax.random.permutation(order_key, SLOTS)
    request_perm = jax.random.permutation(request_key, REQS).astype(jnp.int32)
    request_at = request_perm[rank_at]
    live_drawn = jax.random.randint(live_key, (SLOTS,), 1, SPAN + 1).astype(jnp.int32)
    live_at = jnp.where(jnp.asarray(rank_at) == 0, SPAN, live_drawn).astype(jnp.int32)
    running = jnp.cumsum(live_at) - live_at
    start_at = running - running[firsts][rank_at]
    page_totals = running[bounds - 1] + live_at[bounds - 1] - running[firsts]
    page_counts = jnp.zeros((REQS,), jnp.int32).at[request_perm].set(page_totals.astype(jnp.int32))
    slot_request = jnp.zeros((SLOTS,), jnp.int32).at[order].set(request_at)
    slot_start = jnp.zeros((SLOTS,), jnp.int32).at[order].set(start_at.astype(jnp.int32))
    slot_live = jnp.zeros((SLOTS,), jnp.int32).at[order].set(live_at)
    device_count = SLOTS // ITEMS
    page_keys = jax.random.split(page_key, device_count)
    local_perm = jax.vmap(lambda one_key: jax.random.permutation(one_key, P_DEV))(page_keys)
    slot_pages = local_perm.reshape(SLOTS, SPAN).astype(jnp.int32)
    return (page_counts, slot_request, slot_start, slot_live, slot_pages)


def draw_queries(key, part):
    array_shape = (REQS, QN, H, LAT + ROPE)
    values = jax.random.truncated_normal(jax.random.fold_in(key, 11), -4.0, 4.0, array_shape, jnp.float32)
    return values.reshape(REQS, QN, H * (LAT + ROPE)).astype(jnp.bfloat16)


def draw_cache(key, part):
    array_shape = (PAGES, PAGE, LAT + ROPE)
    values = jax.random.truncated_normal(jax.random.fold_in(key, 22), -4.0, 4.0, array_shape, jnp.float32)
    return values.astype(jnp.bfloat16)


def draw_page_counts(key, part):
    return plan_tables(key)[0]


def draw_slot_request(key, part):
    return plan_tables(key)[1]


def draw_slot_start(key, part):
    return plan_tables(key)[2]


def draw_slot_live(key, part):
    return plan_tables(key)[3]


def draw_slot_pages(key, part):
    return plan_tables(key)[4]


def setup_inputs(seed: int = 0, part: int = 0) -> dict:
    streams_of = jax.random.split(jax.random.key(seed), 8)
    own_keys = jax.random.split(jax.random.fold_in(streams_of[7], part), 8)
    return {
        "queries": draw_queries(jax.random.fold_in(jax.random.fold_in(streams_of[7], part), 71), part),
        "cache": draw_cache(jax.random.fold_in(jax.random.fold_in(streams_of[7], part), 71), part),
        "page_counts": draw_page_counts(jax.random.fold_in(jax.random.fold_in(streams_of[7], part), 71), part),
        "slot_request": draw_slot_request(jax.random.fold_in(jax.random.fold_in(streams_of[7], part), 71), part),
        "slot_start": draw_slot_start(jax.random.fold_in(jax.random.fold_in(streams_of[7], part), 71), part),
        "slot_live": draw_slot_live(jax.random.fold_in(jax.random.fold_in(streams_of[7], part), 71), part),
        "slot_pages": draw_slot_pages(jax.random.fold_in(jax.random.fold_in(streams_of[7], part), 71), part),
    }


softmax_scale = 192.0 ** -0.5
neg_floor = -1.0e30


def slot_partials(query_heads, key_rows, request, first_page, live_pages, page_counts, page_rows, latent):
    row_count = key_rows.shape[1]
    query_count = query_heads.shape[1]
    chosen = query_heads[request].astype(jnp.float32)
    scores = jnp.einsum("gqhc,gjc->gqhj", chosen, key_rows.astype(jnp.float32)) * softmax_scale
    row_ids = jnp.arange(row_count, dtype=jnp.int32)
    page_of = row_ids // page_rows
    position = (first_page[:, None] + page_of[None, :]) * page_rows + row_ids[None, :] % page_rows
    request_pages = page_counts[request]
    query_ids = jnp.arange(query_count, dtype=jnp.int32)
    limit = request_pages[:, None] * page_rows - (query_count - 1 - query_ids)[None, :]
    visible = (page_of[None, None, :] < live_pages[:, None, None]) & (position[:, None, :] < limit[:, :, None])
    visible = visible[:, :, None, :]
    slot_max = jnp.max(jnp.where(visible, scores, neg_floor), axis=3)
    shifted = jnp.where(visible, scores - slot_max[..., None], neg_floor)
    weights = jnp.exp(shifted)
    slot_sum = jnp.sum(weights, axis=3)
    rounded = weights.astype(jnp.bfloat16)
    slot_out = jnp.einsum("gqhj,gjc->gqhc", rounded.astype(jnp.float32), key_rows[:, :, :latent].astype(jnp.float32))
    return slot_max, slot_sum, slot_out


def fold_slots(carry, request, slot_max, slot_sum, slot_out):
    best, denom, numer = carry
    request_count = best.shape[0]
    member = request[:, None] == jnp.arange(request_count, dtype=jnp.int32)[None, :]
    block_best = jnp.max(jnp.where(member[:, :, None, None], slot_max[:, None], neg_floor), axis=0)
    new_best = jnp.maximum(best, block_best)
    kept = jnp.exp(best - new_best)
    member_float = member.astype(jnp.float32)
    factor = jnp.exp(slot_max - new_best[request])
    denom = denom * kept + jnp.einsum("gr,gqh->rqh", member_float, factor * slot_sum, precision=lax.Precision.HIGHEST)
    numer = numer * kept[..., None] + jnp.einsum("gr,gqhc->rqhc", member_float, factor[..., None] * slot_out, precision=lax.Precision.HIGHEST)
    return new_best, denom, numer


def reference(queries, cache, page_counts, slot_request, slot_start, slot_live, slot_pages):
    request_count, query_count, _flat = queries.shape
    token_width = LAT + ROPE
    query_heads = queries.reshape(request_count, query_count, H, token_width)
    owner_base = (jnp.arange(SLOTS, dtype=jnp.int32) // ITEMS) * P_DEV
    global_pages = (slot_pages + owner_base[:, None]).astype(jnp.int32)
    step_count = SLOTS // ITEMS
    inputs = (slot_request.reshape(step_count, ITEMS), slot_start.reshape(step_count, ITEMS),
              slot_live.reshape(step_count, ITEMS), global_pages.reshape(step_count, ITEMS, SPAN))
    initial = (jnp.full((request_count, query_count, H), neg_floor, jnp.float32),
               jnp.zeros((request_count, query_count, H), jnp.float32),
               jnp.zeros((request_count, query_count, H, LAT), jnp.float32))

    def one_step(carry, pieces):
        request, first_page, live_pages, pages = pieces
        key_rows = cache[pages.reshape(-1)].reshape(ITEMS, SPAN * PAGE, token_width)
        slot_max, slot_sum, slot_out = slot_partials(query_heads, key_rows, request, first_page, live_pages, page_counts, PAGE, LAT)
        dev_best, dev_denom, dev_numer = fold_slots(initial, request, slot_max, slot_sum, slot_out)
        dev_partial = lax.optimization_barrier(dev_numer.astype(jnp.bfloat16)).astype(jnp.float32)
        best, denom, numer = carry
        new_best = jnp.maximum(best, dev_best)
        kept = jnp.exp(best - new_best)
        added = jnp.exp(dev_best - new_best)
        denom = denom * kept + dev_denom * added
        numer = numer * kept[..., None] + dev_partial * added[..., None]
        return (new_best, denom, numer), None

    (best, denom, numer), _unused = lax.scan(one_step, initial, inputs)
    attended = (numer / denom[..., None]).reshape(request_count, query_count, H * LAT).astype(jnp.bfloat16)
    lse = best + jnp.log(denom)
    return attended, lse
```

```python
import functools

import jax
import jax.numpy as jnp
from jax import lax
from jax.experimental import pallas as pl
from jax.experimental.pallas import tpu as pltpu
from jax.sharding import PartitionSpec as P

ROPE = 64
CORES = 2
LANES = 128
softmax_scale = 192.0 ** (-0.5)
neg_floor = -1e30
slot_group = 4
vmem_limit = 56 * 1024 * 1024


def place(chip_rows):
    index = lax.axis_index("kv")
    z = index // (2 * CORES)
    y = (index // CORES) % 2
    core = index % CORES
    return index, z, y, core


def device_of(z, y, core):
    return (z * 2 + y) * CORES + core


def gather_kernel(rows_z, x_ref, o_ref, local_sem, send_sems, recv_sems):
    index, z, y, core = place(rows_z)
    other_y, other_core = 1 - y, 1 - core
    has_up, has_down = z < rows_z - 1, z > 0
    barrier = pltpu.get_barrier_semaphore()

    def greet(target):
        pl.semaphore_signal(barrier, inc=1, device_id={"kv": target})

    pl.when(has_up)(lambda: greet(device_of(z + 1, y, core)))
    pl.when(has_down)(lambda: greet(device_of(z - 1, y, core)))
    greet(device_of(z, other_y, core))
    greet(device_of(z, y, other_core))
    pl.semaphore_wait(barrier, 2 + has_up.astype(jnp.int32) + has_down.astype(jnp.int32))

    def copy(slot, way, source=None):
        target = (
            device_of(jnp.minimum(z + 1, rows_z - 1), y, core),
            device_of(jnp.maximum(z - 1, 0), y, core),
            device_of(z, other_y, core),
            device_of(z, y, other_core),
        )[way]
        return pltpu.make_async_remote_copy(
            src_ref=o_ref.at[slot] if source is None else source,
            dst_ref=o_ref.at[slot],
            send_sem=send_sems.at[slot, way],
            recv_sem=recv_sems.at[slot],
            device_id={"kv": target},
        )

    own = pltpu.make_async_copy(x_ref, o_ref.at[index], local_sem)
    own.start()
    pl.when(has_up)(lambda: copy(index, 0, x_ref).start())
    pl.when(has_down)(lambda: copy(index, 1, x_ref).start())
    copy(index, 2, x_ref).start()
    copy(index, 3, x_ref).start()

    def from_below(step):
        slot = device_of(z - step, y, core)
        copy(slot, 3).wait_recv()
        pl.when(has_up)(lambda: copy(slot, 0).start())
        copy(slot, 2).start()
        copy(slot, 3).start()

    def from_above(step):
        slot = device_of(z + step, y, core)
        copy(slot, 3).wait_recv()
        pl.when(has_down)(lambda: copy(slot, 1).start())
        copy(slot, 2).start()
        copy(slot, 3).start()

    def across(row):
        slot = device_of(row, other_y, core)
        copy(slot, 3).wait_recv()
        copy(slot, 3).start()

    def across_pair(step):
        if step == 0:
            across(z)
        else:
            pl.when(z >= step)(lambda: across(z - step))
            pl.when(z + step < rows_z)(lambda: across(z + step))

    for step in range(1, rows_z):
        pl.when(z >= step)(functools.partial(from_below, step))
        pl.when(z + step < rows_z)(functools.partial(from_above, step))
        across_pair(step - 1)
    across_pair(rows_z - 1)
    for row in range(rows_z):
        for column in range(2):
            copy(device_of(row, column, other_core), 3).wait_recv()

    own.wait()
    for row in range(rows_z):
        slot = device_of(row, y, core)
        pl.when(has_up & (row <= z))(lambda slot=slot: copy(slot, 0).wait_send())
        pl.when(has_down & (row >= z))(lambda slot=slot: copy(slot, 1).wait_send())
        copy(slot, 2).wait_send()
        copy(slot, 3).wait_send()
        copy(device_of(row, other_y, core), 3).wait_send()


def gather_queries(shard, rows_z):
    count = rows_z * 2 * CORES
    return pl.pallas_call(
        functools.partial(gather_kernel, rows_z),
        out_shape=jax.ShapeDtypeStruct((count,) + shard.shape, shard.dtype),
        in_specs=[pl.BlockSpec(memory_space=pl.ANY)],
        out_specs=pl.BlockSpec(memory_space=pl.ANY),
        scratch_shapes=[
            pltpu.SemaphoreType.DMA,
            pltpu.SemaphoreType.DMA((count, 4)),
            pltpu.SemaphoreType.DMA((count,)),
        ],
        compiler_params=pltpu.CompilerParams(collective_id=0, has_side_effects=True),
        name="gather_queries",
    )(shard)


def attend_kernel(
    latent, query_count, counts, request, start, live, pages, q_ref, cache_ref, numer_ref, best_ref,
    denom_ref
):
    slots, span = pages.shape
    page_rows = cache_ref.shape[1]
    rows = q_ref.shape[1]
    heads = rows // query_count
    keys = span * page_rows
    best_ref[...] = jnp.full(best_ref.shape, neg_floor, jnp.float32)
    denom_ref[...] = jnp.zeros(denom_ref.shape, jnp.float32)
    numer_ref[...] = jnp.zeros(numer_ref.shape, jnp.float32)
    key_ids = lax.broadcasted_iota(jnp.int32, (rows, keys), 1)
    query_ids = lax.broadcasted_iota(jnp.int32, (rows, keys), 0) // heads

    def group(block, carry):
        parts = []
        for offset in range(slot_group):
            slot = block * slot_group + offset
            r = request[slot]
            key_rows = jnp.concatenate([cache_ref[pages[slot, k]] for k in range(span)], axis=0)
            scores = (
                lax.dot_general(
                    q_ref[r], key_rows, (((1,), (1,)), ((), ())),
                    preferred_element_type=jnp.float32,
                )
                * softmax_scale
            )
            bound = (counts[r] - start[slot]) * page_rows - (query_count - 1)
            visible = (key_ids < live[slot] * page_rows) & (key_ids - query_ids < bound)
            top = jnp.max(jnp.where(visible, scores, neg_floor), axis=1, keepdims=True)
            weights = jnp.where(visible, jnp.exp(scores - top), 0.0)
            total = jnp.sum(weights, axis=1, keepdims=True)
            out = jnp.dot(
                weights.astype(jnp.bfloat16), key_rows[:, :latent],
                preferred_element_type=jnp.float32,
            )
            parts.append((r, top, total, out))
        for r, top, total, out in parts:
            old = best_ref[r]
            new = jnp.maximum(old, top)
            kept = jnp.exp(old - new)
            factor = jnp.exp(top - new)
            best_ref[r] = new
            denom_ref[r] = denom_ref[r] * kept + factor * total
            for first in range(0, latent, LANES):
                columns = slice(first, first + LANES)
                numer_ref[r, :, columns] = (
                    numer_ref[r, :, columns] * kept + out[:, columns] * factor
                )
        return carry

    lax.fori_loop(0, slots // slot_group, group, 0)


def attend(queries, cache, counts, request, start, live, pages, latent, query_count):
    requests, rows, _width = queries.shape
    smem = pl.BlockSpec(memory_space=pltpu.SMEM)
    vmem = pl.BlockSpec(memory_space=pltpu.VMEM)
    return pl.pallas_call(
        functools.partial(attend_kernel, latent, query_count),
        out_shape=(
            jax.ShapeDtypeStruct((requests, rows, latent), jnp.float32),
            jax.ShapeDtypeStruct((requests, rows, LANES), jnp.float32),
            jax.ShapeDtypeStruct((requests, rows, LANES), jnp.float32),
        ),
        in_specs=[smem] * 5 + [vmem] * 2,
        out_specs=(vmem, vmem, vmem),
        compiler_params=pltpu.CompilerParams(vmem_limit_bytes=vmem_limit),
        name="attend",
    )(counts, request, start, live, pages, queries, cache)


def stats_kernel(rows_z, in_ref, out_ref, core_buf, y_buf, z_buf, core_sems, y_sems, z_sems, z_recv):
    index, z, y, core = place(rows_z)
    barrier = pltpu.get_barrier_semaphore()
    others = [device_of(z, y, 1 - core), device_of(z, 1 - y, core)]
    others += [device_of((z + step) % rows_z, y, core) for step in range(1, rows_z)]
    for target in others:
        pl.semaphore_signal(barrier, inc=1, device_id={"kv": target})
    pl.semaphore_wait(barrier, len(others))

    def combine(buf, count):
        top = buf[0, 0]
        for item in range(1, count):
            top = jnp.maximum(top, buf[item, 0])
        total = buf[0, 1] * jnp.exp(buf[0, 0] - top)
        for item in range(1, count):
            total = total + buf[item, 1] * jnp.exp(buf[item, 0] - top)
        return top, total

    def swap(buf, sems, me, target):
        copy = pltpu.make_async_remote_copy(
            src_ref=buf.at[me], dst_ref=buf.at[me], send_sem=sems.at[0], recv_sem=sems.at[1],
            device_id={"kv": target},
        )
        copy.start()
        copy.wait()

    core_buf[core] = in_ref[...]
    swap(core_buf, core_sems, core, others[0])
    top, total = combine(core_buf, CORES)
    y_buf[y, 0] = top
    y_buf[y, 1] = total
    swap(y_buf, y_sems, y, others[1])
    top, total = combine(y_buf, 2)
    z_buf[z, 0] = top
    z_buf[z, 1] = total

    def z_copy(step, source):
        return pltpu.make_async_remote_copy(
            src_ref=z_buf.at[source], dst_ref=z_buf.at[source], send_sem=z_sems.at[step],
            recv_sem=z_recv.at[source], device_id={"kv": device_of((z + step) % rows_z, y, core)},
        )

    for step in range(1, rows_z):
        z_copy(step, z).start()
    for step in range(1, rows_z):
        z_copy(step, (z + step) % rows_z).wait_recv()
    for step in range(1, rows_z):
        z_copy(step, z).wait_send()
    top, total = combine(z_buf, rows_z)
    out_ref[0] = top
    out_ref[1] = total


def combine_stats(stats, rows_z):
    vmem = pl.BlockSpec(memory_space=pltpu.VMEM)
    return pl.pallas_call(
        functools.partial(stats_kernel, rows_z),
        out_shape=jax.ShapeDtypeStruct(stats.shape, stats.dtype),
        in_specs=[vmem],
        out_specs=vmem,
        scratch_shapes=[
            pltpu.VMEM((CORES,) + stats.shape, stats.dtype),
            pltpu.VMEM((2,) + stats.shape, stats.dtype),
            pltpu.VMEM((rows_z,) + stats.shape, stats.dtype),
            pltpu.SemaphoreType.DMA((2,)),
            pltpu.SemaphoreType.DMA((2,)),
            pltpu.SemaphoreType.DMA((rows_z,)),
            pltpu.SemaphoreType.DMA((rows_z,)),
        ],
        compiler_params=pltpu.CompilerParams(collective_id=1, has_side_effects=True),
        name="combine_stats",
    )(stats)


def reduce_kernel(
    rows_z, x_ref, out_ref, core_in, y_out, y_in, z_out, z_in, core_send, core_recv, y_send, y_recv,
    z_send, z_recv
):
    index, z, y, core = place(rows_z)
    other_y, other_core = 1 - y, 1 - core
    partner, across = device_of(z, y, other_core), device_of(z, other_y, core)
    barrier = pltpu.get_barrier_semaphore()
    others = [partner, across]
    others += [device_of((z + step) % rows_z, y, core) for step in range(1, rows_z)]
    for target in others:
        pl.semaphore_signal(barrier, inc=1, device_id={"kv": target})
    pl.semaphore_wait(barrier, len(others))

    def row_of(step):
        return (z + step) % rows_z

    steps = list(range(1, rows_z)) + [0]

    def core_copy(side, step):
        column = other_y if side == 0 else y
        return pltpu.make_async_remote_copy(
            src_ref=x_ref.at[device_of(row_of(step), column, other_core)],
            dst_ref=core_in.at[side, step],
            send_sem=core_send.at[side, step],
            recv_sem=core_recv.at[side, step],
            device_id={"kv": partner},
        )

    def y_copy(step):
        return pltpu.make_async_remote_copy(
            src_ref=y_out.at[step], dst_ref=y_in.at[step], send_sem=y_send.at[step],
            recv_sem=y_recv.at[step], device_id={"kv": across},
        )

    def z_copy(step):
        return pltpu.make_async_remote_copy(
            src_ref=z_out.at[step], dst_ref=z_in.at[step], send_sem=z_send.at[step],
            recv_sem=z_recv.at[step],
            device_id={"kv": device_of(row_of(step), y, core)},
        )

    for side in range(2):
        for step in steps:
            core_copy(side, step).start()

    def wide(value):
        return value.astype(jnp.float32)

    for step in steps:
        core_copy(0, step).wait_recv()
        mine = x_ref[device_of(row_of(step), other_y, core)]
        y_out[step] = (wide(mine) + wide(core_in[0, step])).astype(y_out.dtype)
        y_copy(step).start()
    for step in steps:
        core_copy(1, step).wait_recv()
        y_copy(step).wait_recv()
        mine = x_ref[device_of(row_of(step), y, core)]
        total = wide(mine) + wide(core_in[1, step]) + wide(y_in[step])
        if step:
            z_out[step] = total.astype(z_out.dtype)
            z_copy(step).start()
        else:
            out_ref[...] = total
    for step in range(1, rows_z):
        z_copy(step).wait_recv()
        out_ref[...] += wide(z_in[step])
    for step in steps:
        core_copy(0, step).wait_send()
        core_copy(1, step).wait_send()
        y_copy(step).wait_send()
        if step:
            z_copy(step).wait_send()


def reduce_partials(parts, rows_z):
    block = parts.shape[1:]
    vmem = pl.BlockSpec(memory_space=pltpu.VMEM)
    dma = pltpu.SemaphoreType.DMA
    return pl.pallas_call(
        functools.partial(reduce_kernel, rows_z),
        out_shape=jax.ShapeDtypeStruct(block, jnp.float32),
        in_specs=[vmem],
        out_specs=vmem,
        scratch_shapes=[
            pltpu.VMEM((2, rows_z) + block, parts.dtype),
            pltpu.VMEM((rows_z,) + block, parts.dtype),
            pltpu.VMEM((rows_z,) + block, parts.dtype),
            pltpu.VMEM((rows_z,) + block, parts.dtype),
            pltpu.VMEM((rows_z,) + block, parts.dtype),
            dma((2, rows_z)),
            dma((2, rows_z)),
            dma((rows_z,)),
            dma((rows_z,)),
            dma((rows_z,)),
            dma((rows_z,)),
        ],
        compiler_params=pltpu.CompilerParams(
            collective_id=2, has_side_effects=True, vmem_limit_bytes=vmem_limit
        ),
        name="reduce_partials",
    )(parts)


def per_device(queries, cache, page_counts, slot_request, slot_start, slot_live, slot_pages):
    count = lax.axis_size("kv")
    requests, query_count, shard_width = queries.shape
    token_width = cache.shape[2]
    latent = token_width - ROPE
    heads = count * shard_width // token_width
    rows = query_count * heads
    rows_z = count // (2 * CORES)
    direct = shard_width % token_width == 0 and rows_z * 2 * CORES == count
    if direct:
        local_heads = shard_width // token_width
        shard = queries.reshape(requests * query_count, shard_width)
        gathered = gather_queries(shard, rows_z)
        heads_first = gathered.reshape(count, requests, query_count, local_heads, token_width)
        query_heads = heads_first.transpose(1, 2, 0, 3, 4).reshape(requests, rows, token_width)
    else:
        gathered = lax.all_gather(queries, "kv", axis=2, tiled=True)
        query_heads = gathered.reshape(requests, rows, token_width)
    numer, best, denom = attend(
        query_heads, cache, page_counts, slot_request, slot_start, slot_live, slot_pages, latent,
        query_count,
    )
    best, denom = best[:, :, 0], denom[:, :, 0]
    if direct and best.size % LANES == 0:
        stats = jnp.stack([best.reshape(-1, LANES), denom.reshape(-1, LANES)])
        merged = combine_stats(stats, rows_z)
        highest, total = merged[0].reshape(requests, rows), merged[1].reshape(requests, rows)
    else:
        highest = lax.pmax(best, "kv")
        total = lax.psum(denom * jnp.exp(best - highest), "kv")
    scaled = numer * jnp.exp(best - highest)[..., None]
    lse = (highest + jnp.log(total)).reshape(requests, query_count, heads)
    total = total.reshape(requests, query_count, heads)
    if direct:
        width = local_heads * latent
        parts = scaled.astype(jnp.bfloat16).reshape(
            requests, query_count, count, local_heads * latent
        )
        parts = parts.transpose(2, 0, 1, 3).reshape(count, requests * query_count, width)
        summed = reduce_partials(parts, rows_z).reshape(requests, query_count, width)
    else:
        flat = lax.optimization_barrier(scaled.reshape(requests * query_count, heads * latent))
        width = heads * latent // count
        summed = lax.psum_scatter(flat, "kv", scatter_dimension=1, tiled=True)
        summed = summed.reshape(requests, query_count, width)
    first_head = lax.axis_index("kv") * width // latent
    picked_heads = max(1, width // latent)
    picked = lax.dynamic_slice_in_dim(total, first_head, picked_heads, 2)
    picked = jnp.repeat(picked, min(width, latent), axis=2)
    return ((summed / picked).astype(jnp.bfloat16), lse)


def solution(mesh):
    in_specs = (
        P("rep", None, "kv"),
        P(("rep", "kv"), None, None),
        P("rep"),
        P(("rep", "kv")),
        P(("rep", "kv")),
        P(("rep", "kv")),
        P(("rep", "kv"), None),
    )
    out_specs = (P("rep", None, "kv"), P("rep", None, None))
    return jax.shard_map(
        per_device, mesh=mesh, in_specs=in_specs, out_specs=out_specs, check_vma=False
    )
```

```python
import functools

import jax
import jax.numpy as jnp
from jax import lax
from jax.experimental import pallas as pl
from jax.experimental.pallas import tpu as pltpu
from jax.sharding import PartitionSpec as P

ROPE = 64
CORES = 2
LANES = 128
softmax_scale = 192.0 ** (-0.5)
neg_floor = -1e30
slot_group = 4
vmem_limit = 56 * 1024 * 1024


def place(chip_rows):
    index = lax.axis_index("kv")
    z = index // (2 * CORES)
    y = (index // CORES) % 2
    core = index % CORES
    return index, z, y, core


def device_of(z, y, core):
    return (z * 2 + y) * CORES + core


def gather_kernel(
    rows_z, x_ref, picks_ref, cache_ref, o_ref, keys_ref, cache_buf, keys_buf, local_sem, load_sem,
    store_sem, send_sems, recv_sems
):
    page_rows = cache_ref.shape[0]
    slots = keys_ref.shape[0]
    span = picks_ref.shape[0] // slots
    pairs = page_rows // 2
    index, z, y, core = place(rows_z)
    other_y, other_core = 1 - y, 1 - core
    has_up, has_down = z < rows_z - 1, z > 0
    barrier = pltpu.get_barrier_semaphore()

    def greet(target):
        pl.semaphore_signal(barrier, inc=1, device_id={"kv": target})

    pl.when(has_up)(lambda: greet(device_of(z + 1, y, core)))
    pl.when(has_down)(lambda: greet(device_of(z - 1, y, core)))
    greet(device_of(z, other_y, core))
    greet(device_of(z, y, other_core))
    pl.semaphore_wait(barrier, 2 + has_up.astype(jnp.int32) + has_down.astype(jnp.int32))

    def copy(slot, way, source=None):
        target = (
            device_of(jnp.minimum(z + 1, rows_z - 1), y, core),
            device_of(jnp.maximum(z - 1, 0), y, core),
            device_of(z, other_y, core),
            device_of(z, y, other_core),
        )[way]
        return pltpu.make_async_remote_copy(
            src_ref=o_ref.at[slot] if source is None else source,
            dst_ref=o_ref.at[slot],
            send_sem=send_sems.at[slot, way],
            recv_sem=recv_sems.at[slot],
            device_id={"kv": target},
        )

    own = pltpu.make_async_copy(x_ref, o_ref.at[index], local_sem)
    own.start()
    pl.when(has_up)(lambda: copy(index, 0, x_ref).start())
    pl.when(has_down)(lambda: copy(index, 1, x_ref).start())
    copy(index, 2, x_ref).start()
    copy(index, 3, x_ref).start()
    load = pltpu.make_async_copy(cache_ref, cache_buf, load_sem)
    load.start()

    def pick(row):
        chosen = lax.dot_general(
            picks_ref[...], cache_buf[row], (((1,), (1,)), ((), ())),
            preferred_element_type=jnp.float32,
        )
        return chosen.reshape(slots, span, chosen.shape[1])

    def pick_pairs(part):
        for pair in range(pairs * part // rows_z, pairs * (part + 1) // rows_z):
            both = jnp.concatenate([pick(2 * pair), pick(2 * pair + 1)], axis=1)
            first = pair * 2 * span
            keys_buf[:, first : first + 2 * span, :] = both.astype(keys_buf.dtype)

    def from_below(step):
        slot = device_of(z - step, y, core)
        copy(slot, 3).wait_recv()
        pl.when(has_up)(lambda: copy(slot, 0).start())
        copy(slot, 2).start()
        copy(slot, 3).start()

    def from_above(step):
        slot = device_of(z + step, y, core)
        copy(slot, 3).wait_recv()
        pl.when(has_down)(lambda: copy(slot, 1).start())
        copy(slot, 2).start()
        copy(slot, 3).start()

    def across(row):
        slot = device_of(row, other_y, core)
        copy(slot, 3).wait_recv()
        copy(slot, 3).start()

    def across_pair(step):
        if step == 0:
            across(z)
        else:
            pl.when(z >= step)(lambda: across(z - step))
            pl.when(z + step < rows_z)(lambda: across(z + step))

    load.wait()
    pick_pairs(0)
    for step in range(1, rows_z):
        pl.when(z >= step)(functools.partial(from_below, step))
        pl.when(z + step < rows_z)(functools.partial(from_above, step))
        across_pair(step - 1)
        pick_pairs(step)
    store = pltpu.make_async_copy(keys_buf, keys_ref, store_sem)
    store.start()
    across_pair(rows_z - 1)
    for row in range(rows_z):
        for column in range(2):
            copy(device_of(row, column, other_core), 3).wait_recv()

    own.wait()
    store.wait()
    for row in range(rows_z):
        slot = device_of(row, y, core)
        pl.when(has_up & (row <= z))(lambda slot=slot: copy(slot, 0).wait_send())
        pl.when(has_down & (row >= z))(lambda slot=slot: copy(slot, 1).wait_send())
        copy(slot, 2).wait_send()
        copy(slot, 3).wait_send()
        copy(device_of(row, other_y, core), 3).wait_send()


def gather_queries(shard, picks, cache, slots, rows_z):
    count = rows_z * 2 * CORES
    page_rows, token_width, _pages = cache.shape
    keys = jax.ShapeDtypeStruct(
        (slots, picks.shape[0] // slots * page_rows, token_width), cache.dtype
    )
    hbm = pl.BlockSpec(memory_space=pl.ANY)
    return pl.pallas_call(
        functools.partial(gather_kernel, rows_z),
        out_shape=(jax.ShapeDtypeStruct((count,) + shard.shape, shard.dtype), keys),
        in_specs=[hbm, pl.BlockSpec(memory_space=pltpu.VMEM), hbm],
        out_specs=(hbm, hbm),
        scratch_shapes=[
            pltpu.VMEM(cache.shape, cache.dtype),
            pltpu.VMEM(keys.shape, keys.dtype),
            pltpu.SemaphoreType.DMA,
            pltpu.SemaphoreType.DMA,
            pltpu.SemaphoreType.DMA,
            pltpu.SemaphoreType.DMA((count, 4)),
            pltpu.SemaphoreType.DMA((count,)),
        ],
        compiler_params=pltpu.CompilerParams(
            collective_id=0, has_side_effects=True, vmem_limit_bytes=vmem_limit
        ),
        name="gather_queries",
    )(shard, picks, cache)


def attend_whole_kernel(
    latent, query_count, counts, request, start, live, pages, q_ref, cache_ref, numer_ref, best_ref,
    denom_ref
):
    slots, span = pages.shape
    page_rows = cache_ref.shape[1]
    rows = q_ref.shape[1]
    heads = rows // query_count
    keys = span * page_rows
    best_ref[...] = jnp.full(best_ref.shape, neg_floor, jnp.float32)
    denom_ref[...] = jnp.zeros(denom_ref.shape, jnp.float32)
    numer_ref[...] = jnp.zeros(numer_ref.shape, jnp.float32)
    key_ids = lax.broadcasted_iota(jnp.int32, (rows, keys), 1)
    query_ids = lax.broadcasted_iota(jnp.int32, (rows, keys), 0) // heads

    def group(block, carry):
        parts = []
        for offset in range(slot_group):
            slot = block * slot_group + offset
            r = request[slot]
            key_rows = jnp.concatenate([cache_ref[pages[slot, k]] for k in range(span)], axis=0)
            scores = (
                lax.dot_general(
                    q_ref[r], key_rows, (((1,), (1,)), ((), ())),
                    preferred_element_type=jnp.float32,
                )
                * softmax_scale
            )
            bound = (counts[r] - start[slot]) * page_rows - (query_count - 1)
            visible = (key_ids < live[slot] * page_rows) & (key_ids - query_ids < bound)
            top = jnp.max(jnp.where(visible, scores, neg_floor), axis=1, keepdims=True)
            weights = jnp.where(visible, jnp.exp(scores - top), 0.0)
            total = jnp.sum(weights, axis=1, keepdims=True)
            out = jnp.dot(
                weights.astype(jnp.bfloat16), key_rows[:, :latent],
                preferred_element_type=jnp.float32,
            )
            parts.append((r, top, total, out))
        for r, top, total, out in parts:
            old = best_ref[r]
            new = jnp.maximum(old, top)
            kept = jnp.exp(old - new)
            factor = jnp.exp(top - new)
            best_ref[r] = new
            denom_ref[r] = denom_ref[r] * kept + factor * total
            for first in range(0, latent, LANES):
                columns = slice(first, first + LANES)
                numer_ref[r, :, columns] = (
                    numer_ref[r, :, columns] * kept + out[:, columns] * factor
                )
        return carry

    lax.fori_loop(0, slots // slot_group, group, 0)


def attend_whole(queries, cache, counts, request, start, live, pages, latent, query_count):
    requests, rows, _width = queries.shape
    smem = pl.BlockSpec(memory_space=pltpu.SMEM)
    vmem = pl.BlockSpec(memory_space=pltpu.VMEM)
    return pl.pallas_call(
        functools.partial(attend_whole_kernel, latent, query_count),
        out_shape=(
            jax.ShapeDtypeStruct((requests, rows, latent), jnp.float32),
            jax.ShapeDtypeStruct((requests, rows, LANES), jnp.float32),
            jax.ShapeDtypeStruct((requests, rows, LANES), jnp.float32),
        ),
        in_specs=[smem] * 5 + [vmem] * 2,
        out_specs=(vmem, vmem, vmem),
        compiler_params=pltpu.CompilerParams(vmem_limit_bytes=vmem_limit),
        name="attend_whole",
    )(counts, request, start, live, pages, queries, cache)


def attend_blocks_kernel(
    query_count, page_rows, counts, request, start, live, q_ref, keys_ref, part_ref, stats_ref,
    wide_q, narrow_q, numer, best, denom
):
    devices, _rows, shard_width = q_ref.shape
    slots, keys, token_width = keys_ref.shape
    latent = part_ref.shape[2]
    requests, rows = narrow_q.shape[0], narrow_q.shape[1]
    heads = rows // query_count
    local_heads = heads // devices
    span = keys // page_rows
    best[...] = jnp.full(best.shape, neg_floor, jnp.float32)
    denom[...] = jnp.zeros(denom.shape, jnp.float32)
    numer[...] = jnp.zeros(numer.shape, jnp.float32)
    chunks = [(c, min(LANES, token_width - c)) for c in range(0, token_width, LANES)]

    def spread(device, carry):
        for i in range(query_count):
            block = q_ref[device, i * requests : (i + 1) * requests, :].astype(jnp.float32)
            for local in range(local_heads):
                row = i * heads + device * local_heads + local
                for c, (first, size) in enumerate(chunks):
                    at = local * token_width + first
                    wide_q[c, pl.ds(row, requests, stride=rows), 0:size] = block[:, at : at + size]
        return carry

    lax.fori_loop(0, devices, spread, 0)

    def narrow(r, carry):
        for c, (first, size) in enumerate(chunks):
            at = pl.multiple_of(r * rows, 64)
            narrow_q[r, :, first : first + size] = wide_q[c, pl.ds(at, rows), 0:size].astype(
                narrow_q.dtype
            )
        return carry

    lax.fori_loop(0, requests, narrow, 0)

    key_ids = lax.broadcasted_iota(jnp.int32, (rows, keys), 1)
    row_in_page = key_ids // (2 * span) * 2 + key_ids % (2 * span) // span
    key_ids = key_ids % span * page_rows + row_in_page
    query_ids = lax.broadcasted_iota(jnp.int32, (rows, keys), 0) // heads
    reach_ids = key_ids - query_ids

    def group(block, carry):
        parts = []
        for offset in range(slot_group):
            slot = block * slot_group + offset
            r = request[slot]
            key_rows = keys_ref[slot]
            scores = (
                lax.dot_general(
                    narrow_q[r], key_rows, (((1,), (1,)), ((), ())),
                    preferred_element_type=jnp.float32,
                )
                * softmax_scale
            )
            bound = (counts[r] - start[slot]) * page_rows - (query_count - 1)
            visible = (key_ids < live[slot] * page_rows) & (reach_ids < bound)
            top = jnp.max(jnp.where(visible, scores, neg_floor), axis=1, keepdims=True)
            weights = jnp.where(visible, jnp.exp(scores - top), 0.0)
            total = jnp.sum(weights, axis=1, keepdims=True)
            out = jnp.dot(
                weights.astype(jnp.bfloat16), key_rows[:, :latent],
                preferred_element_type=jnp.float32,
            )
            parts.append((r, top, total, out))
        for r, top, total, out in parts:
            at = pl.ds(pl.multiple_of(r * rows, 64), rows)
            old = best[at, :]
            new = jnp.maximum(old, top)
            kept = jnp.exp(old - new)
            factor = jnp.exp(top - new)
            best[at, :] = new
            denom[at, :] = denom[at, :] * kept + factor * total
            for c in range(latent // LANES):
                columns = out[:, c * LANES : (c + 1) * LANES]
                numer[c, at, :] = numer[c, at, :] * kept + columns * factor
        return carry

    lax.fori_loop(0, slots // slot_group, group, 0)

    def hand_out(device, carry):
        tops, totals = [], []
        for local in range(local_heads):
            for i in range(query_count):
                at = pl.ds(i * heads + device * local_heads + local, requests, stride=rows)
                first = (local * query_count + i) * requests
                tops.append(best[at, :])
                totals.append(denom[at, :])
                for c in range(latent // LANES):
                    part_ref[
                        device, first : first + requests, c * LANES : (c + 1) * LANES
                    ] = numer[c, at, :].astype(part_ref.dtype)
        stats_ref[0, pl.ds(device, 1), :] = jnp.concatenate(tops, axis=0).T[0:1, :]
        stats_ref[1, pl.ds(device, 1), :] = jnp.concatenate(totals, axis=0).T[0:1, :]
        return carry

    lax.fori_loop(0, devices, hand_out, 0)


def attend_blocks(queries, keys, counts, request, start, live, query_count, page_rows, latent):
    devices, query_rows, shard_width = queries.shape
    requests = query_rows // query_count
    token_width = keys.shape[2]
    rows = query_count * devices * shard_width // token_width
    block_rows = requests * rows // devices
    smem = pl.BlockSpec(memory_space=pltpu.SMEM)
    vmem = pl.BlockSpec(memory_space=pltpu.VMEM)
    wide = jnp.float32
    return pl.pallas_call(
        functools.partial(attend_blocks_kernel, query_count, page_rows),
        out_shape=(
            jax.ShapeDtypeStruct((devices, block_rows, latent), jnp.bfloat16),
            jax.ShapeDtypeStruct((2, devices, block_rows), wide),
        ),
        in_specs=[smem] * 4 + [vmem] * 2,
        out_specs=(vmem, vmem),
        scratch_shapes=[
            pltpu.VMEM((-(-token_width // LANES), requests * rows, LANES), wide),
            pltpu.VMEM((requests, rows, token_width), queries.dtype),
            pltpu.VMEM((latent // LANES, requests * rows, LANES), wide),
            pltpu.VMEM((requests * rows, LANES), wide),
            pltpu.VMEM((requests * rows, LANES), wide),
        ],
        compiler_params=pltpu.CompilerParams(vmem_limit_bytes=vmem_limit),
        name="attend_blocks",
    )(counts, request, start, live, queries, keys)


def combine(buf, count):
    top = buf[0, 0]
    for item in range(1, count):
        top = jnp.maximum(top, buf[item, 0])
    total = buf[0, 1] * jnp.exp(buf[0, 0] - top)
    for item in range(1, count):
        total = total + buf[item, 1] * jnp.exp(buf[item, 0] - top)
    return top, total


def reduce_kernel(
    rows_z, query_count, x_ref, stats_ref, out_ref, lse_ref, core_in, y_out, y_in, z_out, z_in,
    core_stats, y_stats, z_stats, factors, totals, core_send, core_recv, y_send, y_recv, z_send,
    z_recv, core_sems, y_sems, zs_send, zs_recv
):
    index, z, y, core = place(rows_z)
    other_y, other_core = 1 - y, 1 - core
    partner, across = device_of(z, y, other_core), device_of(z, other_y, core)
    block_rows = x_ref.shape[1]
    barrier = pltpu.get_barrier_semaphore()
    others = [partner, across]
    others += [device_of((z + step) % rows_z, y, core) for step in range(1, rows_z)]
    for target in others:
        pl.semaphore_signal(barrier, inc=1, device_id={"kv": target})
    pl.semaphore_wait(barrier, len(others))

    def row_of(step):
        return (z + step) % rows_z

    steps = list(range(1, rows_z)) + [0]

    def core_copy(side, step):
        column = other_y if side == 0 else y
        return pltpu.make_async_remote_copy(
            src_ref=x_ref.at[device_of(row_of(step), column, other_core)],
            dst_ref=core_in.at[side, step],
            send_sem=core_send.at[side, step],
            recv_sem=core_recv.at[side, step],
            device_id={"kv": partner},
        )

    def y_copy(step):
        return pltpu.make_async_remote_copy(
            src_ref=y_out.at[step], dst_ref=y_in.at[step], send_sem=y_send.at[step],
            recv_sem=y_recv.at[step], device_id={"kv": across},
        )

    def z_copy(step):
        return pltpu.make_async_remote_copy(
            src_ref=z_out.at[step], dst_ref=z_in.at[step], send_sem=z_send.at[step],
            recv_sem=z_recv.at[step],
            device_id={"kv": device_of(row_of(step), y, core)},
        )

    def swap(buf, sems, me, target):
        copy = pltpu.make_async_remote_copy(
            src_ref=buf.at[me], dst_ref=buf.at[me], send_sem=sems.at[0], recv_sem=sems.at[1],
            device_id={"kv": target},
        )
        copy.start()
        return copy

    def stats_copy(step, source):
        return pltpu.make_async_remote_copy(
            src_ref=z_stats.at[source], dst_ref=z_stats.at[source], send_sem=zs_send.at[step],
            recv_sem=zs_recv.at[source], device_id={"kv": device_of(row_of(step), y, core)},
        )

    core_stats[core] = stats_ref[...]
    swapped = swap(core_stats, core_sems, core, partner)
    for side in range(2):
        for step in steps:
            core_copy(side, step).start()
    swapped.wait()
    y_stats[y, 0], y_stats[y, 1] = combine(core_stats, CORES)
    swap(y_stats, y_sems, y, across).wait()
    z_stats[z, 0], z_stats[z, 1] = combine(y_stats, 2)
    for step in range(1, rows_z):
        stats_copy(step, z).start()
    for step in range(1, rows_z):
        stats_copy(step, row_of(step)).wait_recv()
    top, total = combine(z_stats, rows_z)
    lse_ref[...] = top + jnp.log(total)
    totals[...] = total
    for side in range(CORES):
        factors[side] = jnp.exp(core_stats[side, 0] - top)

    def down(row):
        return jnp.broadcast_to(row, (LANES, block_rows)).T

    def scaled(value, side, target):
        spread = down(factors[side, pl.ds(target, 1), :])
        wide = value.astype(jnp.float32)
        return wide * jnp.concatenate([spread] * (wide.shape[1] // LANES), axis=1)

    def both(side, step):
        target = device_of(row_of(step), other_y if side == 0 else y, core)
        core_copy(side, step).wait_recv()
        return scaled(x_ref[target], core, target) + scaled(
            core_in[side, step], other_core, target
        )

    for step in steps:
        y_out[step] = both(0, step).astype(y_out.dtype)
        y_copy(step).start()
    for step in steps:
        total = both(1, step)
        y_copy(step).wait_recv()
        total = total + y_in[step].astype(jnp.float32)
        if step:
            z_out[step] = total.astype(z_out.dtype)
            z_copy(step).start()
    for step in range(1, rows_z):
        z_copy(step).wait_recv()
        total = total + z_in[step].astype(jnp.float32)
    over = down(totals[pl.ds(index, 1), :])
    total = total / jnp.concatenate([over] * (total.shape[1] // LANES), axis=1)
    width = total.shape[1]
    local_rows = out_ref.shape[0]
    for local in range(block_rows // local_rows):
        out_ref[:, local * width : (local + 1) * width] = total[
            local * local_rows : (local + 1) * local_rows
        ].astype(out_ref.dtype)
    for step in range(1, rows_z):
        stats_copy(step, z).wait_send()
    for step in steps:
        core_copy(0, step).wait_send()
        core_copy(1, step).wait_send()
        y_copy(step).wait_send()
        if step:
            z_copy(step).wait_send()


def reduce_partials(parts, stats, rows_z, query_rows, query_count):
    block = parts.shape[1:]
    vmem = pl.BlockSpec(memory_space=pltpu.VMEM)
    dma = pltpu.SemaphoreType.DMA
    width = block[0] // query_rows * block[1]
    return pl.pallas_call(
        functools.partial(reduce_kernel, rows_z, query_count),
        out_shape=(
            jax.ShapeDtypeStruct((query_rows, width), jnp.bfloat16),
            jax.ShapeDtypeStruct(stats.shape[1:], jnp.float32),
        ),
        in_specs=[vmem, vmem],
        out_specs=(vmem, vmem),
        scratch_shapes=[
            pltpu.VMEM((2, rows_z) + block, parts.dtype),
            pltpu.VMEM((rows_z,) + block, parts.dtype),
            pltpu.VMEM((rows_z,) + block, parts.dtype),
            pltpu.VMEM((rows_z,) + block, parts.dtype),
            pltpu.VMEM((rows_z,) + block, parts.dtype),
            pltpu.VMEM((CORES,) + stats.shape, jnp.float32),
            pltpu.VMEM((2,) + stats.shape, jnp.float32),
            pltpu.VMEM((rows_z,) + stats.shape, jnp.float32),
            pltpu.VMEM((CORES,) + stats.shape[1:], jnp.float32),
            pltpu.VMEM(stats.shape[1:], jnp.float32),
            dma((2, rows_z)),
            dma((2, rows_z)),
            dma((rows_z,)),
            dma((rows_z,)),
            dma((rows_z,)),
            dma((rows_z,)),
            dma((2,)),
            dma((2,)),
            dma((rows_z,)),
            dma((rows_z,)),
        ],
        compiler_params=pltpu.CompilerParams(
            collective_id=2, has_side_effects=True, vmem_limit_bytes=vmem_limit
        ),
        name="reduce_partials",
    )(parts, stats)


def per_device(queries, cache, page_counts, slot_request, slot_start, slot_live, slot_pages):
    count = lax.axis_size("kv")
    requests, query_count, shard_width = queries.shape
    page_rows, token_width = cache.shape[1:]
    latent = token_width - ROPE
    heads = count * shard_width // token_width
    rows_z = count // (2 * CORES)
    slots = slot_request.shape[0]
    if shard_width % token_width or rows_z * 2 * CORES != count:
        return per_device_whole(
            queries, cache, page_counts, slot_request, slot_start, slot_live, slot_pages
        )
    local_heads = shard_width // token_width
    query_rows = query_count * requests
    shard = queries.transpose(1, 0, 2).reshape(query_rows, shard_width)
    page_ids = jnp.arange(cache.shape[0], dtype=jnp.int32)
    picks = (slot_pages.reshape(-1, 1) == page_ids[None, :]).astype(cache.dtype)
    gathered, keys = gather_queries(shard, picks, cache.transpose(1, 2, 0), slots, rows_z)
    parts, stats = attend_blocks(
        gathered, keys, page_counts, slot_request, slot_start, slot_live, query_count, page_rows,
        latent,
    )
    attended, lse = reduce_partials(parts, stats, rows_z, query_rows, query_count)
    attended = attended.reshape(query_count, requests, local_heads * latent).transpose(1, 0, 2)
    lse = lse.reshape(count * local_heads, query_count, requests).transpose(2, 1, 0)
    return (attended, lse)


def per_device_whole(queries, cache, page_counts, slot_request, slot_start, slot_live, slot_pages):
    count = lax.axis_size("kv")
    requests, query_count, shard_width = queries.shape
    token_width = cache.shape[2]
    latent = token_width - ROPE
    heads = count * shard_width // token_width
    rows = query_count * heads
    gathered = lax.all_gather(queries, "kv", axis=2, tiled=True)
    query_heads = gathered.reshape(requests, rows, token_width)
    numer, best, denom = attend_whole(
        query_heads, cache, page_counts, slot_request, slot_start, slot_live, slot_pages, latent,
        query_count,
    )
    best, denom = best[:, :, 0], denom[:, :, 0]
    highest = lax.pmax(best, "kv")
    total = lax.psum(denom * jnp.exp(best - highest), "kv")
    scaled = numer * jnp.exp(best - highest)[..., None]
    lse = (highest + jnp.log(total)).reshape(requests, query_count, heads)
    total = total.reshape(requests, query_count, heads)
    flat = lax.optimization_barrier(scaled.reshape(requests * query_count, heads * latent))
    width = heads * latent // count
    summed = lax.psum_scatter(flat, "kv", scatter_dimension=1, tiled=True)
    summed = summed.reshape(requests, query_count, width)
    first_head = lax.axis_index("kv") * width // latent
    picked_heads = max(1, width // latent)
    picked = lax.dynamic_slice_in_dim(total, first_head, picked_heads, 2)
    picked = jnp.repeat(picked, min(width, latent), axis=2)
    return ((summed / picked).astype(jnp.bfloat16), lse)


def solution(mesh):
    in_specs = (
        P("rep", None, "kv"),
        P(("rep", "kv"), None, None),
        P("rep"),
        P(("rep", "kv")),
        P(("rep", "kv")),
        P(("rep", "kv")),
        P(("rep", "kv"), None),
    )
    out_specs = (P("rep", None, "kv"), P("rep", None, None))
    return jax.shard_map(
        per_device, mesh=mesh, in_specs=in_specs, out_specs=out_specs, check_vma=False
    )
```

```python
import functools

import jax
import jax.numpy as jnp
from jax import lax
from jax.experimental import pallas as pl
from jax.experimental.pallas import tpu as pltpu
from jax.sharding import PartitionSpec as P

ROPE = 64
CORES = 2
LANES = 128
softmax_scale = 192.0 ** (-0.5)
neg_floor = -1e30
slot_group = 4
vmem_limit = 56 * 1024 * 1024


def place(chip_rows):
    index = lax.axis_index("kv")
    z = index // (2 * CORES)
    y = (index // CORES) % 2
    core = index % CORES
    return index, z, y, core


def device_of(z, y, core):
    return (z * 2 + y) * CORES + core


def gather_kernel(
    rows_z, query_count, x_ref, picks_ref, cache_ref, q_ref, keys_ref, o_ref, wide_q, narrow_q,
    cache_buf, keys_buf, local_sem, load_sem, store_sem, q_sems, send_sems, recv_sems
):
    devices, query_rows, shard_width = o_ref.shape
    requests, rows, token_width = narrow_q.shape
    heads = rows // query_count
    local_heads = heads // devices
    chunks = [(c, min(LANES, token_width - c)) for c in range(0, token_width, LANES)]
    page_rows = cache_ref.shape[0]
    slots = keys_ref.shape[0]
    span = picks_ref.shape[0] // slots
    pairs = page_rows // 2
    index, z, y, core = place(rows_z)
    other_y, other_core = 1 - y, 1 - core
    has_up, has_down = z < rows_z - 1, z > 0
    barrier = pltpu.get_barrier_semaphore()

    def greet(target):
        pl.semaphore_signal(barrier, inc=1, device_id={"kv": target})

    pl.when(has_up)(lambda: greet(device_of(z + 1, y, core)))
    pl.when(has_down)(lambda: greet(device_of(z - 1, y, core)))
    greet(device_of(z, other_y, core))
    greet(device_of(z, y, other_core))
    pl.semaphore_wait(barrier, 2 + has_up.astype(jnp.int32) + has_down.astype(jnp.int32))

    def copy(slot, way, source=None):
        target = (
            device_of(jnp.minimum(z + 1, rows_z - 1), y, core),
            device_of(jnp.maximum(z - 1, 0), y, core),
            device_of(z, other_y, core),
            device_of(z, y, other_core),
        )[way]
        return pltpu.make_async_remote_copy(
            src_ref=o_ref.at[slot] if source is None else source,
            dst_ref=o_ref.at[slot],
            send_sem=send_sems.at[slot, way],
            recv_sem=recv_sems.at[slot],
            device_id={"kv": target},
        )

    own = pltpu.make_async_copy(x_ref, o_ref.at[index], local_sem)
    own.start()
    pl.when(has_up)(lambda: copy(index, 0, x_ref).start())
    pl.when(has_down)(lambda: copy(index, 1, x_ref).start())
    copy(index, 2, x_ref).start()
    copy(index, 3, x_ref).start()
    load = pltpu.make_async_copy(cache_ref, cache_buf, load_sem)
    load.start()

    def pick(row):
        chosen = lax.dot_general(
            picks_ref[...], cache_buf[row], (((1,), (1,)), ((), ())),
            preferred_element_type=jnp.float32,
        )
        return chosen.reshape(slots, span, chosen.shape[1])

    def pick_pairs(part):
        for pair in range(pairs * part // rows_z, pairs * (part + 1) // rows_z):
            both = jnp.concatenate([pick(2 * pair), pick(2 * pair + 1)], axis=1)
            first = pair * 2 * span
            keys_buf[:, first : first + 2 * span, :] = both.astype(keys_buf.dtype)

    def from_below(step):
        slot = device_of(z - step, y, core)
        copy(slot, 3).wait_recv()
        pl.when(has_up)(lambda: copy(slot, 0).start())
        copy(slot, 2).start()
        copy(slot, 3).start()

    def from_above(step):
        slot = device_of(z + step, y, core)
        copy(slot, 3).wait_recv()
        pl.when(has_down)(lambda: copy(slot, 1).start())
        copy(slot, 2).start()
        copy(slot, 3).start()

    def across(row):
        slot = device_of(row, other_y, core)
        copy(slot, 3).wait_recv()
        copy(slot, 3).start()

    def across_pair(step):
        if step == 0:
            across(z)
        else:
            pl.when(z >= step)(lambda: across(z - step))
            pl.when(z + step < rows_z)(lambda: across(z + step))

    def spread(device):
        def one_query(i, carry):
            at = pl.ds(pl.multiple_of(i * requests, requests), requests)
            block = o_ref[device, at, :].astype(jnp.float32)
            for local in range(local_heads):
                to = pl.ds(i * heads + device * local_heads + local, requests, stride=rows)
                for c, (first, size) in enumerate(chunks):
                    begin = local * token_width + first
                    wide_q[c, to, 0:size] = block[:, begin : begin + size]
            return carry

        lax.fori_loop(0, query_count, one_query, 0)

    def arrange(column, step):
        def pair(row):
            spread(device_of(row, column, core))
            copy(device_of(row, column, other_core), 3).wait_recv()
            spread(device_of(row, column, other_core))

        if step == 0:
            pair(z)
        else:
            pl.when(z >= step)(lambda: pair(z - step))
            pl.when(z + step < rows_z)(lambda: pair(z + step))

    load.wait()
    pick_pairs(0)
    own.wait()
    for step in range(1, rows_z):
        pl.when(z >= step)(functools.partial(from_below, step))
        pl.when(z + step < rows_z)(functools.partial(from_above, step))
        across_pair(step - 1)
        pick_pairs(step)
        arrange(y, step - 1)
        if step > 1:
            arrange(other_y, step - 2)
    store = pltpu.make_async_copy(keys_buf, keys_ref, store_sem)
    store.start()
    across_pair(rows_z - 1)
    arrange(y, rows_z - 1)
    if rows_z > 1:
        arrange(other_y, rows_z - 2)
    arrange(other_y, rows_z - 1)

    def hand_on(r):
        return pltpu.make_async_copy(narrow_q.at[r], q_ref.at[r], q_sems.at[r])

    def narrow(r, carry):
        at = pl.ds(pl.multiple_of(r * rows, 64), rows)
        for c, (first, size) in enumerate(chunks):
            narrow_q[r, :, first : first + size] = wide_q[c, at, 0:size].astype(narrow_q.dtype)
        hand_on(r).start()
        return carry

    lax.fori_loop(0, requests, narrow, 0)
    store.wait()
    for r in range(requests):
        hand_on(r).wait()
    for row in range(rows_z):
        slot = device_of(row, y, core)
        pl.when(has_up & (row <= z))(lambda slot=slot: copy(slot, 0).wait_send())
        pl.when(has_down & (row >= z))(lambda slot=slot: copy(slot, 1).wait_send())
        copy(slot, 2).wait_send()
        copy(slot, 3).wait_send()
        copy(device_of(row, other_y, core), 3).wait_send()


def gather_queries(shard, picks, cache, slots, rows_z, query_count):
    count = rows_z * 2 * CORES
    page_rows, token_width, _pages = cache.shape
    requests = shard.shape[0] // query_count
    rows = query_count * count * shard.shape[1] // token_width
    keys = jax.ShapeDtypeStruct(
        (slots, picks.shape[0] // slots * page_rows, token_width), cache.dtype
    )
    grouped = jax.ShapeDtypeStruct((requests, rows, token_width), shard.dtype)
    hbm = pl.BlockSpec(memory_space=pl.ANY)
    return pl.pallas_call(
        functools.partial(gather_kernel, rows_z, query_count),
        out_shape=(grouped, keys),
        in_specs=[hbm, pl.BlockSpec(memory_space=pltpu.VMEM), hbm],
        out_specs=(hbm, hbm),
        scratch_shapes=[
            pltpu.VMEM((count,) + shard.shape, shard.dtype),
            pltpu.VMEM((-(-token_width // LANES), requests * rows, LANES), jnp.float32),
            pltpu.VMEM(grouped.shape, grouped.dtype),
            pltpu.VMEM(cache.shape, cache.dtype),
            pltpu.VMEM(keys.shape, keys.dtype),
            pltpu.SemaphoreType.DMA,
            pltpu.SemaphoreType.DMA,
            pltpu.SemaphoreType.DMA,
            pltpu.SemaphoreType.DMA((requests,)),
            pltpu.SemaphoreType.DMA((count, 4)),
            pltpu.SemaphoreType.DMA((count,)),
        ],
        compiler_params=pltpu.CompilerParams(
            collective_id=0, has_side_effects=True, vmem_limit_bytes=vmem_limit
        ),
        name="gather_queries",
    )(shard, picks, cache)


def attend_whole_kernel(
    latent, query_count, counts, request, start, live, pages, q_ref, cache_ref, numer_ref, best_ref,
    denom_ref
):
    slots, span = pages.shape
    page_rows = cache_ref.shape[1]
    rows = q_ref.shape[1]
    heads = rows // query_count
    keys = span * page_rows
    best_ref[...] = jnp.full(best_ref.shape, neg_floor, jnp.float32)
    denom_ref[...] = jnp.zeros(denom_ref.shape, jnp.float32)
    numer_ref[...] = jnp.zeros(numer_ref.shape, jnp.float32)
    key_ids = lax.broadcasted_iota(jnp.int32, (rows, keys), 1)
    query_ids = lax.broadcasted_iota(jnp.int32, (rows, keys), 0) // heads

    def group(block, carry):
        parts = []
        for offset in range(slot_group):
            slot = block * slot_group + offset
            r = request[slot]
            key_rows = jnp.concatenate([cache_ref[pages[slot, k]] for k in range(span)], axis=0)
            scores = (
                lax.dot_general(
                    q_ref[r], key_rows, (((1,), (1,)), ((), ())),
                    preferred_element_type=jnp.float32,
                )
                * softmax_scale
            )
            bound = (counts[r] - start[slot]) * page_rows - (query_count - 1)
            visible = (key_ids < live[slot] * page_rows) & (key_ids - query_ids < bound)
            top = jnp.max(jnp.where(visible, scores, neg_floor), axis=1, keepdims=True)
            weights = jnp.where(visible, jnp.exp(scores - top), 0.0)
            total = jnp.sum(weights, axis=1, keepdims=True)
            out = jnp.dot(
                weights.astype(jnp.bfloat16), key_rows[:, :latent],
                preferred_element_type=jnp.float32,
            )
            parts.append((r, top, total, out))
        for r, top, total, out in parts:
            old = best_ref[r]
            new = jnp.maximum(old, top)
            kept = jnp.exp(old - new)
            factor = jnp.exp(top - new)
            best_ref[r] = new
            denom_ref[r] = denom_ref[r] * kept + factor * total
            for first in range(0, latent, LANES):
                columns = slice(first, first + LANES)
                numer_ref[r, :, columns] = (
                    numer_ref[r, :, columns] * kept + out[:, columns] * factor
                )
        return carry

    lax.fori_loop(0, slots // slot_group, group, 0)


def attend_whole(queries, cache, counts, request, start, live, pages, latent, query_count):
    requests, rows, _width = queries.shape
    smem = pl.BlockSpec(memory_space=pltpu.SMEM)
    vmem = pl.BlockSpec(memory_space=pltpu.VMEM)
    return pl.pallas_call(
        functools.partial(attend_whole_kernel, latent, query_count),
        out_shape=(
            jax.ShapeDtypeStruct((requests, rows, latent), jnp.float32),
            jax.ShapeDtypeStruct((requests, rows, LANES), jnp.float32),
            jax.ShapeDtypeStruct((requests, rows, LANES), jnp.float32),
        ),
        in_specs=[smem] * 5 + [vmem] * 2,
        out_specs=(vmem, vmem, vmem),
        compiler_params=pltpu.CompilerParams(vmem_limit_bytes=vmem_limit),
        name="attend_whole",
    )(counts, request, start, live, pages, queries, cache)


def attend_blocks_kernel(
    query_count, page_rows, counts, request, start, live, q_hbm, keys_hbm, part_hbm, stats_ref,
    narrow_q, keys_ref, part_ref, numer, best, denom, q_sem, key_sems, part_sems
):
    devices = part_ref.shape[0]
    slots, keys, token_width = keys_ref.shape
    latent = part_ref.shape[2]
    queries_in = pltpu.make_async_copy(q_hbm, narrow_q, q_sem)
    queries_in.start()

    def keys_in(block):
        at = pl.ds(block * slot_group, slot_group)
        return pltpu.make_async_copy(keys_hbm.at[at], keys_ref.at[at], key_sems.at[block])

    def part_out(device):
        return pltpu.make_async_copy(
            part_ref.at[device], part_hbm.at[device], part_sems.at[device]
        )

    for block in range(slots // slot_group):
        keys_in(block).start()
    requests, rows = narrow_q.shape[0], narrow_q.shape[1]
    heads = rows // query_count
    local_heads = heads // devices
    span = keys // page_rows
    best[...] = jnp.full(best.shape, neg_floor, jnp.float32)
    denom[...] = jnp.zeros(denom.shape, jnp.float32)
    numer[...] = jnp.zeros(numer.shape, jnp.float32)
    key_ids = lax.broadcasted_iota(jnp.int32, (rows, keys), 1)
    row_in_page = key_ids // (2 * span) * 2 + key_ids % (2 * span) // span
    key_ids = key_ids % span * page_rows + row_in_page
    query_ids = lax.broadcasted_iota(jnp.int32, (rows, keys), 0) // heads
    reach_ids = key_ids - query_ids
    queries_in.wait()

    def group(block, carry):
        parts = []
        keys_in(block).wait()
        for offset in range(slot_group):
            slot = block * slot_group + offset
            r = request[slot]
            key_rows = keys_ref[slot]
            scores = (
                lax.dot_general(
                    narrow_q[r], key_rows, (((1,), (1,)), ((), ())),
                    preferred_element_type=jnp.float32,
                )
                * softmax_scale
            )
            bound = (counts[r] - start[slot]) * page_rows - (query_count - 1)
            visible = (key_ids < live[slot] * page_rows) & (reach_ids < bound)
            top = jnp.max(jnp.where(visible, scores, neg_floor), axis=1, keepdims=True)
            weights = jnp.where(visible, jnp.exp(scores - top), 0.0)
            total = jnp.sum(weights, axis=1, keepdims=True)
            out = jnp.dot(
                weights.astype(jnp.bfloat16), key_rows[:, :latent],
                preferred_element_type=jnp.float32,
            )
            parts.append((r, top, total, out))
        for r, top, total, out in parts:
            at = pl.ds(pl.multiple_of(r * rows, 64), rows)
            old = best[at, :]
            new = jnp.maximum(old, top)
            kept = jnp.exp(old - new)
            factor = jnp.exp(top - new)
            best[at, :] = new
            denom[at, :] = denom[at, :] * kept + factor * total
            for c in range(latent // LANES):
                columns = out[:, c * LANES : (c + 1) * LANES]
                numer[c, at, :] = numer[c, at, :] * kept + columns * factor
        return carry

    lax.fori_loop(0, slots // slot_group, group, 0)

    def hand_out(device, carry):
        tops, totals = [], []
        for local in range(local_heads):
            for i in range(query_count):
                at = pl.ds(i * heads + device * local_heads + local, requests, stride=rows)
                first = (local * query_count + i) * requests
                tops.append(best[at, :])
                totals.append(denom[at, :])
                for c in range(latent // LANES):
                    part_ref[
                        device, first : first + requests, c * LANES : (c + 1) * LANES
                    ] = numer[c, at, :].astype(part_ref.dtype)
        stats_ref[0, pl.ds(device, 1), :] = jnp.concatenate(tops, axis=0).T[0:1, :]
        part_out(device).start()
        stats_ref[1, pl.ds(device, 1), :] = jnp.concatenate(totals, axis=0).T[0:1, :]
        return carry

    lax.fori_loop(0, devices, hand_out, 0)
    for device in range(devices):
        part_out(device).wait()


def attend_blocks(
    queries, keys, counts, request, start, live, devices, query_count, page_rows, latent
):
    requests, rows, token_width = queries.shape
    block_rows = requests * rows // devices
    smem = pl.BlockSpec(memory_space=pltpu.SMEM)
    vmem = pl.BlockSpec(memory_space=pltpu.VMEM)
    hbm = pl.BlockSpec(memory_space=pl.ANY)
    dma = pltpu.SemaphoreType.DMA
    wide = jnp.float32
    return pl.pallas_call(
        functools.partial(attend_blocks_kernel, query_count, page_rows),
        out_shape=(
            jax.ShapeDtypeStruct((devices, block_rows, latent), jnp.bfloat16),
            jax.ShapeDtypeStruct((2, devices, block_rows), wide),
        ),
        in_specs=[smem] * 4 + [hbm] * 2,
        out_specs=(hbm, vmem),
        scratch_shapes=[
            pltpu.VMEM(queries.shape, queries.dtype),
            pltpu.VMEM(keys.shape, keys.dtype),
            pltpu.VMEM((devices, block_rows, latent), jnp.bfloat16),
            pltpu.VMEM((latent // LANES, requests * rows, LANES), wide),
            pltpu.VMEM((requests * rows, LANES), wide),
            pltpu.VMEM((requests * rows, LANES), wide),
            dma,
            dma((keys.shape[0] // slot_group,)),
            dma((devices,)),
        ],
        compiler_params=pltpu.CompilerParams(vmem_limit_bytes=vmem_limit),
        name="attend_blocks",
    )(counts, request, start, live, queries, keys)


def combine(buf, count):
    top = buf[0, 0]
    for item in range(1, count):
        top = jnp.maximum(top, buf[item, 0])
    total = buf[0, 1] * jnp.exp(buf[0, 0] - top)
    for item in range(1, count):
        total = total + buf[item, 1] * jnp.exp(buf[item, 0] - top)
    return top, total


def reduce_kernel(
    rows_z, x_hbm, stats_ref, out_ref, lse_ref, x_ref, x_sems, core_in, y_out, y_in, z_out, z_in,
    core_stats, y_stats, z_stats, factors, totals, core_send, core_recv, y_send, y_recv, z_send,
    z_recv, core_sems, y_sems, zs_send, zs_recv
):
    index, z, y, core = place(rows_z)
    other_y, other_core = 1 - y, 1 - core
    partner, across = device_of(z, y, other_core), device_of(z, other_y, core)
    block_rows = x_ref.shape[2]
    barrier = pltpu.get_barrier_semaphore()
    others = [partner, across]
    others += [device_of((z + step) % rows_z, y, core) for step in range(1, rows_z)]
    for target in others:
        pl.semaphore_signal(barrier, inc=1, device_id={"kv": target})
    pl.semaphore_wait(barrier, len(others))

    def row_of(step):
        return (z + step) % rows_z

    steps = list(range(1, rows_z)) + [0]

    def core_copy(side, step):
        column = other_y if side == 0 else y
        return pltpu.make_async_remote_copy(
            src_ref=x_hbm.at[device_of(row_of(step), column, other_core)],
            dst_ref=core_in.at[side, step],
            send_sem=core_send.at[side, step],
            recv_sem=core_recv.at[side, step],
            device_id={"kv": partner},
        )

    def y_copy(step):
        return pltpu.make_async_remote_copy(
            src_ref=y_out.at[step], dst_ref=y_in.at[step], send_sem=y_send.at[step],
            recv_sem=y_recv.at[step], device_id={"kv": across},
        )

    def z_copy(step):
        return pltpu.make_async_remote_copy(
            src_ref=z_out.at[step], dst_ref=z_in.at[step], send_sem=z_send.at[step],
            recv_sem=z_recv.at[step],
            device_id={"kv": device_of(row_of(step), y, core)},
        )

    def swap(buf, sems, me, target):
        copy = pltpu.make_async_remote_copy(
            src_ref=buf.at[me], dst_ref=buf.at[me], send_sem=sems.at[0], recv_sem=sems.at[1],
            device_id={"kv": target},
        )
        copy.start()
        return copy

    def stats_copy(step, source):
        return pltpu.make_async_remote_copy(
            src_ref=z_stats.at[source], dst_ref=z_stats.at[source], send_sem=zs_send.at[step],
            recv_sem=zs_recv.at[source], device_id={"kv": device_of(row_of(step), y, core)},
        )

    def x_copy(side, step):
        column = other_y if side == 0 else y
        return pltpu.make_async_copy(
            x_hbm.at[device_of(row_of(step), column, core)], x_ref.at[side, step],
            x_sems.at[side, step],
        )

    core_stats[core] = stats_ref[...]
    swapped = swap(core_stats, core_sems, core, partner)
    for side in range(2):
        for step in steps:
            core_copy(side, step).start()
    for side in range(2):
        for step in steps:
            x_copy(side, step).start()
    swapped.wait()
    y_stats[y, 0], y_stats[y, 1] = combine(core_stats, CORES)
    swap(y_stats, y_sems, y, across).wait()
    z_stats[z, 0], z_stats[z, 1] = combine(y_stats, 2)
    for step in range(1, rows_z):
        stats_copy(step, z).start()
    for step in range(1, rows_z):
        stats_copy(step, row_of(step)).wait_recv()
    top, total = combine(z_stats, rows_z)
    lse_ref[...] = top + jnp.log(total)
    totals[...] = total
    for side in range(CORES):
        factors[side] = jnp.exp(core_stats[side, 0] - top)

    def down(row):
        return jnp.broadcast_to(row, (LANES, block_rows)).T

    def scaled(value, side, target):
        spread = down(factors[side, pl.ds(target, 1), :])
        wide = value.astype(jnp.float32)
        return wide * jnp.concatenate([spread] * (wide.shape[1] // LANES), axis=1)

    def both(side, step):
        target = device_of(row_of(step), other_y if side == 0 else y, core)
        x_copy(side, step).wait()
        core_copy(side, step).wait_recv()
        return scaled(x_ref[side, step], core, target) + scaled(
            core_in[side, step], other_core, target
        )

    for step in steps:
        y_out[step] = both(0, step).astype(y_out.dtype)
        y_copy(step).start()
    for step in steps:
        total = both(1, step)
        y_copy(step).wait_recv()
        total = total + y_in[step].astype(jnp.float32)
        if step:
            z_out[step] = total.astype(z_out.dtype)
            z_copy(step).start()
    for step in range(1, rows_z):
        z_copy(step).wait_recv()
        total = total + z_in[step].astype(jnp.float32)
    over = down(totals[pl.ds(index, 1), :])
    total = total / jnp.concatenate([over] * (total.shape[1] // LANES), axis=1)
    width = total.shape[1]
    local_rows = out_ref.shape[0]
    for local in range(block_rows // local_rows):
        out_ref[:, local * width : (local + 1) * width] = total[
            local * local_rows : (local + 1) * local_rows
        ].astype(out_ref.dtype)
    for step in range(1, rows_z):
        stats_copy(step, z).wait_send()
    for step in steps:
        core_copy(0, step).wait_send()
        core_copy(1, step).wait_send()
        y_copy(step).wait_send()
        if step:
            z_copy(step).wait_send()


def reduce_partials(parts, stats, rows_z, query_rows):
    block = parts.shape[1:]
    vmem = pl.BlockSpec(memory_space=pltpu.VMEM)
    dma = pltpu.SemaphoreType.DMA
    width = block[0] // query_rows * block[1]
    return pl.pallas_call(
        functools.partial(reduce_kernel, rows_z),
        out_shape=(
            jax.ShapeDtypeStruct((query_rows, width), jnp.bfloat16),
            jax.ShapeDtypeStruct(stats.shape[1:], jnp.float32),
        ),
        in_specs=[pl.BlockSpec(memory_space=pl.ANY), vmem],
        out_specs=(vmem, vmem),
        scratch_shapes=[
            pltpu.VMEM((2, rows_z) + block, parts.dtype),
            dma((2, rows_z)),
            pltpu.VMEM((2, rows_z) + block, parts.dtype),
            pltpu.VMEM((rows_z,) + block, parts.dtype),
            pltpu.VMEM((rows_z,) + block, parts.dtype),
            pltpu.VMEM((rows_z,) + block, parts.dtype),
            pltpu.VMEM((rows_z,) + block, parts.dtype),
            pltpu.VMEM((CORES,) + stats.shape, jnp.float32),
            pltpu.VMEM((2,) + stats.shape, jnp.float32),
            pltpu.VMEM((rows_z,) + stats.shape, jnp.float32),
            pltpu.VMEM((CORES,) + stats.shape[1:], jnp.float32),
            pltpu.VMEM(stats.shape[1:], jnp.float32),
            dma((2, rows_z)),
            dma((2, rows_z)),
            dma((rows_z,)),
            dma((rows_z,)),
            dma((rows_z,)),
            dma((rows_z,)),
            dma((2,)),
            dma((2,)),
            dma((rows_z,)),
            dma((rows_z,)),
        ],
        compiler_params=pltpu.CompilerParams(
            collective_id=2, has_side_effects=True, vmem_limit_bytes=vmem_limit
        ),
        name="reduce_partials",
    )(parts, stats)


def per_device(queries, cache, page_counts, slot_request, slot_start, slot_live, slot_pages):
    count = lax.axis_size("kv")
    requests, query_count, shard_width = queries.shape
    page_rows, token_width = cache.shape[1:]
    latent = token_width - ROPE
    heads = count * shard_width // token_width
    rows_z = count // (2 * CORES)
    slots = slot_request.shape[0]
    if shard_width % token_width or rows_z * 2 * CORES != count:
        return per_device_whole(
            queries, cache, page_counts, slot_request, slot_start, slot_live, slot_pages
        )
    local_heads = shard_width // token_width
    query_rows = query_count * requests
    shard = queries.transpose(1, 0, 2).reshape(query_rows, shard_width)
    page_ids = jnp.arange(cache.shape[0], dtype=jnp.int32)
    picks = (slot_pages.reshape(-1, 1) == page_ids[None, :]).astype(cache.dtype)
    gathered, keys = gather_queries(
        shard, picks, cache.transpose(1, 2, 0), slots, rows_z, query_count
    )
    parts, stats = attend_blocks(
        gathered, keys, page_counts, slot_request, slot_start, slot_live, count, query_count,
        page_rows, latent,
    )
    attended, lse = reduce_partials(parts, stats, rows_z, query_rows)
    attended = attended.reshape(query_count, requests, local_heads * latent).transpose(1, 0, 2)
    lse = lse.reshape(count * local_heads, query_count, requests).transpose(2, 1, 0)
    return (attended, lse)


def per_device_whole(queries, cache, page_counts, slot_request, slot_start, slot_live, slot_pages):
    count = lax.axis_size("kv")
    requests, query_count, shard_width = queries.shape
    token_width = cache.shape[2]
    latent = token_width - ROPE
    heads = count * shard_width // token_width
    rows = query_count * heads
    gathered = lax.all_gather(queries, "kv", axis=2, tiled=True)
    query_heads = gathered.reshape(requests, rows, token_width)
    numer, best, denom = attend_whole(
        query_heads, cache, page_counts, slot_request, slot_start, slot_live, slot_pages, latent,
        query_count,
    )
    best, denom = best[:, :, 0], denom[:, :, 0]
    highest = lax.pmax(best, "kv")
    total = lax.psum(denom * jnp.exp(best - highest), "kv")
    scaled = numer * jnp.exp(best - highest)[..., None]
    lse = (highest + jnp.log(total)).reshape(requests, query_count, heads)
    total = total.reshape(requests, query_count, heads)
    flat = lax.optimization_barrier(scaled.reshape(requests * query_count, heads * latent))
    width = heads * latent // count
    summed = lax.psum_scatter(flat, "kv", scatter_dimension=1, tiled=True)
    summed = summed.reshape(requests, query_count, width)
    first_head = lax.axis_index("kv") * width // latent
    picked_heads = max(1, width // latent)
    picked = lax.dynamic_slice_in_dim(total, first_head, picked_heads, 2)
    picked = jnp.repeat(picked, min(width, latent), axis=2)
    return ((summed / picked).astype(jnp.bfloat16), lse)


def solution(mesh):
    in_specs = (
        P("rep", None, "kv"),
        P(("rep", "kv"), None, None),
        P("rep"),
        P(("rep", "kv")),
        P(("rep", "kv")),
        P(("rep", "kv")),
        P(("rep", "kv"), None),
    )
    out_specs = (P("rep", None, "kv"), P("rep", None, None))
    return jax.shard_map(
        per_device, mesh=mesh, in_specs=in_specs, out_specs=out_specs, check_vma=False
    )
```

```python
import functools

import jax
import jax.numpy as jnp
from jax import lax
from jax.experimental import pallas as pl
from jax.experimental.pallas import tpu as pltpu
from jax.sharding import PartitionSpec as P

ROPE = 64
CORES = 2
LANES = 128
softmax_scale = 192.0 ** (-0.5)
neg_floor = -1e30
slot_group = 8
vmem_limit = 56 * 1024 * 1024


def place(chip_rows):
    index = lax.axis_index("kv")
    z = index // (2 * CORES)
    y = (index // CORES) % 2
    core = index % CORES
    return index, z, y, core


def device_of(z, y, core):
    return (z * 2 + y) * CORES + core


def gather_kernel(
    rows_z, query_count, x_ref, picks_ref, cache_ref, q_ref, keys_ref, o_ref, wide_q, narrow_q,
    cache_buf, keys_buf, local_sem, load_sem, store_sem, q_sems, send_sems, recv_sems
):
    devices, query_rows, shard_width = o_ref.shape
    requests, rows, token_width = narrow_q.shape
    heads = rows // query_count
    local_heads = heads // devices
    chunks = [(c, min(LANES, token_width - c)) for c in range(0, token_width, LANES)]
    page_rows = cache_ref.shape[0]
    slots = keys_ref.shape[0]
    span = picks_ref.shape[0] // slots
    pairs = page_rows // 2
    index, z, y, core = place(rows_z)
    other_y, other_core = 1 - y, 1 - core
    has_up, has_down = z < rows_z - 1, z > 0
    barrier = pltpu.get_barrier_semaphore()

    def greet(target):
        pl.semaphore_signal(barrier, inc=1, device_id={"kv": target})

    pl.when(has_up)(lambda: greet(device_of(z + 1, y, core)))
    pl.when(has_down)(lambda: greet(device_of(z - 1, y, core)))
    greet(device_of(z, other_y, core))
    greet(device_of(z, y, other_core))
    pl.semaphore_wait(barrier, 2 + has_up.astype(jnp.int32) + has_down.astype(jnp.int32))

    def copy(slot, way, source=None):
        target = (
            device_of(jnp.minimum(z + 1, rows_z - 1), y, core),
            device_of(jnp.maximum(z - 1, 0), y, core),
            device_of(z, other_y, core),
            device_of(z, y, other_core),
        )[way]
        return pltpu.make_async_remote_copy(
            src_ref=o_ref.at[slot] if source is None else source,
            dst_ref=o_ref.at[slot],
            send_sem=send_sems.at[slot, way],
            recv_sem=recv_sems.at[slot],
            device_id={"kv": target},
        )

    own = pltpu.make_async_copy(x_ref, o_ref.at[index], local_sem)
    own.start()
    pl.when(has_up)(lambda: copy(index, 0, x_ref).start())
    pl.when(has_down)(lambda: copy(index, 1, x_ref).start())
    copy(index, 2, x_ref).start()
    copy(index, 3, x_ref).start()
    load = pltpu.make_async_copy(cache_ref, cache_buf, load_sem)
    load.start()

    def pick(row):
        chosen = lax.dot_general(
            picks_ref[...], cache_buf[row], (((1,), (1,)), ((), ())),
            preferred_element_type=jnp.float32,
        )
        return chosen.reshape(slots, span, chosen.shape[1])

    def pick_pairs(part):
        for pair in range(pairs * part // rows_z, pairs * (part + 1) // rows_z):
            both = jnp.concatenate([pick(2 * pair), pick(2 * pair + 1)], axis=1)
            first = pair * 2 * span
            keys_buf[:, first : first + 2 * span, :] = both.astype(keys_buf.dtype)

    def from_below(step):
        slot = device_of(z - step, y, core)
        copy(slot, 3).wait_recv()
        pl.when(has_up)(lambda: copy(slot, 0).start())
        copy(slot, 2).start()
        copy(slot, 3).start()

    def from_above(step):
        slot = device_of(z + step, y, core)
        copy(slot, 3).wait_recv()
        pl.when(has_down)(lambda: copy(slot, 1).start())
        copy(slot, 2).start()
        copy(slot, 3).start()

    def across(row):
        slot = device_of(row, other_y, core)
        copy(slot, 3).wait_recv()
        copy(slot, 3).start()

    def across_pair(step):
        if step == 0:
            across(z)
        else:
            pl.when(z >= step)(lambda: across(z - step))
            pl.when(z + step < rows_z)(lambda: across(z + step))

    def spread(device):
        def one_query(i, carry):
            at = pl.ds(pl.multiple_of(i * requests, requests), requests)
            block = o_ref[device, at, :].astype(jnp.float32)
            for local in range(local_heads):
                to = pl.ds(i * heads + device * local_heads + local, requests, stride=rows)
                for c, (first, size) in enumerate(chunks):
                    begin = local * token_width + first
                    wide_q[c, to, 0:size] = block[:, begin : begin + size]
            return carry

        lax.fori_loop(0, query_count, one_query, 0)

    def arrange(column, step):
        def pair(row):
            spread(device_of(row, column, core))
            copy(device_of(row, column, other_core), 3).wait_recv()
            spread(device_of(row, column, other_core))

        if step == 0:
            pair(z)
        else:
            pl.when(z >= step)(lambda: pair(z - step))
            pl.when(z + step < rows_z)(lambda: pair(z + step))

    load.wait()
    pick_pairs(0)
    own.wait()
    for step in range(1, rows_z):
        pl.when(z >= step)(functools.partial(from_below, step))
        pl.when(z + step < rows_z)(functools.partial(from_above, step))
        across_pair(step - 1)
        pick_pairs(step)
        arrange(y, step - 1)
        if step > 1:
            arrange(other_y, step - 2)
    store = pltpu.make_async_copy(keys_buf, keys_ref, store_sem)
    store.start()
    across_pair(rows_z - 1)
    arrange(y, rows_z - 1)
    if rows_z > 1:
        arrange(other_y, rows_z - 2)
    arrange(other_y, rows_z - 1)

    def hand_on(r):
        return pltpu.make_async_copy(narrow_q.at[r], q_ref.at[r], q_sems.at[r])

    def narrow(r, carry):
        at = pl.ds(pl.multiple_of(r * rows, 64), rows)
        for c, (first, size) in enumerate(chunks):
            narrow_q[r, :, first : first + size] = wide_q[c, at, 0:size].astype(narrow_q.dtype)
        hand_on(r).start()
        return carry

    lax.fori_loop(0, requests, narrow, 0)
    store.wait()
    for r in range(requests):
        hand_on(r).wait()
    for row in range(rows_z):
        slot = device_of(row, y, core)
        pl.when(has_up & (row <= z))(lambda slot=slot: copy(slot, 0).wait_send())
        pl.when(has_down & (row >= z))(lambda slot=slot: copy(slot, 1).wait_send())
        copy(slot, 2).wait_send()
        copy(slot, 3).wait_send()
        copy(device_of(row, other_y, core), 3).wait_send()


def gather_queries(shard, picks, cache, slots, rows_z, query_count):
    count = rows_z * 2 * CORES
    page_rows, token_width, _pages = cache.shape
    requests = shard.shape[0] // query_count
    rows = query_count * count * shard.shape[1] // token_width
    keys = jax.ShapeDtypeStruct(
        (slots, picks.shape[0] // slots * page_rows, token_width), cache.dtype
    )
    grouped = jax.ShapeDtypeStruct((requests, rows, token_width), shard.dtype)
    hbm = pl.BlockSpec(memory_space=pl.ANY)
    return pl.pallas_call(
        functools.partial(gather_kernel, rows_z, query_count),
        out_shape=(grouped, keys),
        in_specs=[hbm, pl.BlockSpec(memory_space=pltpu.VMEM), hbm],
        out_specs=(hbm, hbm),
        scratch_shapes=[
            pltpu.VMEM((count,) + shard.shape, shard.dtype),
            pltpu.VMEM((-(-token_width // LANES), requests * rows, LANES), jnp.float32),
            pltpu.VMEM(grouped.shape, grouped.dtype),
            pltpu.VMEM(cache.shape, cache.dtype),
            pltpu.VMEM(keys.shape, keys.dtype),
            pltpu.SemaphoreType.DMA,
            pltpu.SemaphoreType.DMA,
            pltpu.SemaphoreType.DMA,
            pltpu.SemaphoreType.DMA((requests,)),
            pltpu.SemaphoreType.DMA((count, 4)),
            pltpu.SemaphoreType.DMA((count,)),
        ],
        compiler_params=pltpu.CompilerParams(
            collective_id=0, has_side_effects=True, vmem_limit_bytes=vmem_limit
        ),
        name="gather_queries",
    )(shard, picks, cache)


def attend_whole_kernel(
    latent, query_count, counts, request, start, live, pages, q_ref, cache_ref, numer_ref, best_ref,
    denom_ref
):
    slots, span = pages.shape
    page_rows = cache_ref.shape[1]
    rows = q_ref.shape[1]
    heads = rows // query_count
    keys = span * page_rows
    best_ref[...] = jnp.full(best_ref.shape, neg_floor, jnp.float32)
    denom_ref[...] = jnp.zeros(denom_ref.shape, jnp.float32)
    numer_ref[...] = jnp.zeros(numer_ref.shape, jnp.float32)
    key_ids = lax.broadcasted_iota(jnp.int32, (rows, keys), 1)
    query_ids = lax.broadcasted_iota(jnp.int32, (rows, keys), 0) // heads

    def group(block, carry):
        parts = []
        for offset in range(slot_group):
            slot = block * slot_group + offset
            r = request[slot]
            key_rows = jnp.concatenate([cache_ref[pages[slot, k]] for k in range(span)], axis=0)
            scores = (
                lax.dot_general(
                    q_ref[r], key_rows, (((1,), (1,)), ((), ())),
                    preferred_element_type=jnp.float32,
                )
                * softmax_scale
            )
            bound = (counts[r] - start[slot]) * page_rows - (query_count - 1)
            visible = (key_ids < live[slot] * page_rows) & (key_ids - query_ids < bound)
            top = jnp.max(jnp.where(visible, scores, neg_floor), axis=1, keepdims=True)
            weights = jnp.where(visible, jnp.exp(scores - top), 0.0)
            total = jnp.sum(weights, axis=1, keepdims=True)
            out = jnp.dot(
                weights.astype(jnp.bfloat16), key_rows[:, :latent],
                preferred_element_type=jnp.float32,
            )
            parts.append((r, top, total, out))
        for r, top, total, out in parts:
            old = best_ref[r]
            new = jnp.maximum(old, top)
            kept = jnp.exp(old - new)
            factor = jnp.exp(top - new)
            best_ref[r] = new
            denom_ref[r] = denom_ref[r] * kept + factor * total
            for first in range(0, latent, LANES):
                columns = slice(first, first + LANES)
                numer_ref[r, :, columns] = (
                    numer_ref[r, :, columns] * kept + out[:, columns] * factor
                )
        return carry

    lax.fori_loop(0, slots // slot_group, group, 0)


def attend_whole(queries, cache, counts, request, start, live, pages, latent, query_count):
    requests, rows, _width = queries.shape
    smem = pl.BlockSpec(memory_space=pltpu.SMEM)
    vmem = pl.BlockSpec(memory_space=pltpu.VMEM)
    return pl.pallas_call(
        functools.partial(attend_whole_kernel, latent, query_count),
        out_shape=(
            jax.ShapeDtypeStruct((requests, rows, latent), jnp.float32),
            jax.ShapeDtypeStruct((requests, rows, LANES), jnp.float32),
            jax.ShapeDtypeStruct((requests, rows, LANES), jnp.float32),
        ),
        in_specs=[smem] * 5 + [vmem] * 2,
        out_specs=(vmem, vmem, vmem),
        compiler_params=pltpu.CompilerParams(vmem_limit_bytes=vmem_limit),
        name="attend_whole",
    )(counts, request, start, live, pages, queries, cache)


def attend_blocks_kernel(
    query_count, page_rows, counts, request, start, live, q_hbm, keys_hbm, part_hbm, stats_ref,
    narrow_q, keys_ref, part_ref, numer, best, denom, q_sem, key_sems, part_sems
):
    devices = part_ref.shape[0]
    slots, keys, token_width = keys_ref.shape
    latent = part_ref.shape[2]
    queries_in = pltpu.make_async_copy(q_hbm, narrow_q, q_sem)
    queries_in.start()

    def keys_in(block):
        at = pl.ds(block * slot_group, slot_group)
        return pltpu.make_async_copy(keys_hbm.at[at], keys_ref.at[at], key_sems.at[block])

    def part_out(device):
        return pltpu.make_async_copy(
            part_ref.at[device], part_hbm.at[device], part_sems.at[device]
        )

    for block in range(slots // slot_group):
        keys_in(block).start()
    requests, rows = narrow_q.shape[0], narrow_q.shape[1]
    heads = rows // query_count
    local_heads = heads // devices
    span = keys // page_rows
    best[...] = jnp.full(best.shape, neg_floor, jnp.float32)
    denom[...] = jnp.zeros(denom.shape, jnp.float32)
    numer[...] = jnp.zeros(numer.shape, jnp.float32)
    key_ids = lax.broadcasted_iota(jnp.int32, (rows, keys), 1)
    row_in_page = key_ids // (2 * span) * 2 + key_ids % (2 * span) // span
    key_ids = key_ids % span * page_rows + row_in_page
    query_ids = lax.broadcasted_iota(jnp.int32, (rows, keys), 0) // heads
    reach_ids = key_ids - query_ids
    queries_in.wait()

    def group(block, carry):
        parts = []
        keys_in(block).wait()
        for offset in range(slot_group):
            slot = block * slot_group + offset
            r = request[slot]
            key_rows = keys_ref[slot]
            scores = (
                lax.dot_general(
                    narrow_q[r], key_rows, (((1,), (1,)), ((), ())),
                    preferred_element_type=jnp.float32,
                )
                * softmax_scale
            )
            bound = (counts[r] - start[slot]) * page_rows - (query_count - 1)
            visible = (key_ids < live[slot] * page_rows) & (reach_ids < bound)
            top = jnp.max(jnp.where(visible, scores, neg_floor), axis=1, keepdims=True)
            weights = jnp.where(visible, jnp.exp(scores - top), 0.0)
            total = jnp.sum(weights, axis=1, keepdims=True)
            out = jnp.dot(
                weights.astype(jnp.bfloat16), key_rows[:, :latent],
                preferred_element_type=jnp.float32,
            )
            parts.append((r, top, total, out))
        for r, top, total, out in parts:
            at = pl.ds(pl.multiple_of(r * rows, 64), rows)
            old = best[at, :]
            new = jnp.maximum(old, top)
            kept = jnp.exp(old - new)
            factor = jnp.exp(top - new)
            best[at, :] = new
            denom[at, :] = denom[at, :] * kept + factor * total
            for c in range(latent // LANES):
                columns = out[:, c * LANES : (c + 1) * LANES]
                numer[c, at, :] = numer[c, at, :] * kept + columns * factor
        return carry

    lax.fori_loop(0, slots // slot_group, group, 0)

    def hand_out(device, carry):
        tops, totals = [], []
        for local in range(local_heads):
            for i in range(query_count):
                at = pl.ds(i * heads + device * local_heads + local, requests, stride=rows)
                first = (local * query_count + i) * requests
                tops.append(best[at, :])
                totals.append(denom[at, :])
                for c in range(latent // LANES):
                    part_ref[
                        device, first : first + requests, c * LANES : (c + 1) * LANES
                    ] = numer[c, at, :].astype(part_ref.dtype)
        stats_ref[0, pl.ds(device, 1), :] = jnp.concatenate(tops, axis=0).T[0:1, :]
        part_out(device).start()
        stats_ref[1, pl.ds(device, 1), :] = jnp.concatenate(totals, axis=0).T[0:1, :]
        return carry

    lax.fori_loop(0, devices, hand_out, 0)
    for device in range(devices):
        part_out(device).wait()


def attend_blocks(
    queries, keys, counts, request, start, live, devices, query_count, page_rows, latent
):
    requests, rows, token_width = queries.shape
    block_rows = requests * rows // devices
    smem = pl.BlockSpec(memory_space=pltpu.SMEM)
    vmem = pl.BlockSpec(memory_space=pltpu.VMEM)
    hbm = pl.BlockSpec(memory_space=pl.ANY)
    dma = pltpu.SemaphoreType.DMA
    wide = jnp.float32
    return pl.pallas_call(
        functools.partial(attend_blocks_kernel, query_count, page_rows),
        out_shape=(
            jax.ShapeDtypeStruct((devices, block_rows, latent), jnp.bfloat16),
            jax.ShapeDtypeStruct((2, devices, block_rows), wide),
        ),
        in_specs=[smem] * 4 + [hbm] * 2,
        out_specs=(hbm, vmem),
        scratch_shapes=[
            pltpu.VMEM(queries.shape, queries.dtype),
            pltpu.VMEM(keys.shape, keys.dtype),
            pltpu.VMEM((devices, block_rows, latent), jnp.bfloat16),
            pltpu.VMEM((latent // LANES, requests * rows, LANES), wide),
            pltpu.VMEM((requests * rows, LANES), wide),
            pltpu.VMEM((requests * rows, LANES), wide),
            dma,
            dma((keys.shape[0] // slot_group,)),
            dma((devices,)),
        ],
        compiler_params=pltpu.CompilerParams(vmem_limit_bytes=vmem_limit),
        name="attend_blocks",
    )(counts, request, start, live, queries, keys)


def combine(buf, count):
    top = buf[0, 0]
    for item in range(1, count):
        top = jnp.maximum(top, buf[item, 0])
    total = buf[0, 1] * jnp.exp(buf[0, 0] - top)
    for item in range(1, count):
        total = total + buf[item, 1] * jnp.exp(buf[item, 0] - top)
    return top, total


def reduce_kernel(
    rows_z, x_hbm, stats_ref, out_ref, lse_ref, x_ref, x_sems, core_in, y_out, y_in, z_out, z_in,
    core_stats, y_stats, z_stats, near, factors, totals, core_send, core_recv, y_send, y_recv, z_send,
    z_recv, core_sems, y_sems, zs_send, zs_recv
):
    index, z, y, core = place(rows_z)
    other_y, other_core = 1 - y, 1 - core
    partner, across = device_of(z, y, other_core), device_of(z, other_y, core)
    block_rows = x_ref.shape[2]
    barrier = pltpu.get_barrier_semaphore()
    others = [partner, across]
    others += [device_of((z + step) % rows_z, y, core) for step in range(1, rows_z)]
    for target in others:
        pl.semaphore_signal(barrier, inc=1, device_id={"kv": target})
    pl.semaphore_wait(barrier, len(others))

    def row_of(step):
        return (z + step) % rows_z

    steps = list(range(1, rows_z)) + [0]

    def core_copy(side, step):
        column = other_y if side == 0 else y
        return pltpu.make_async_remote_copy(
            src_ref=x_hbm.at[device_of(row_of(step), column, other_core)],
            dst_ref=core_in.at[side, step],
            send_sem=core_send.at[side, step],
            recv_sem=core_recv.at[side, step],
            device_id={"kv": partner},
        )

    def y_copy(step):
        return pltpu.make_async_remote_copy(
            src_ref=y_out.at[step], dst_ref=y_in.at[step], send_sem=y_send.at[step],
            recv_sem=y_recv.at[step], device_id={"kv": across},
        )

    def z_copy(step):
        return pltpu.make_async_remote_copy(
            src_ref=z_out.at[step], dst_ref=z_in.at[step], send_sem=z_send.at[step],
            recv_sem=z_recv.at[step],
            device_id={"kv": device_of(row_of(step), y, core)},
        )

    def swap(buf, sems, me, target):
        copy = pltpu.make_async_remote_copy(
            src_ref=buf.at[me], dst_ref=buf.at[me], send_sem=sems.at[0], recv_sem=sems.at[1],
            device_id={"kv": target},
        )
        copy.start()
        return copy

    def stats_copy(step, source):
        return pltpu.make_async_remote_copy(
            src_ref=z_stats.at[source], dst_ref=z_stats.at[source], send_sem=zs_send.at[step],
            recv_sem=zs_recv.at[source], device_id={"kv": device_of(row_of(step), y, core)},
        )

    def x_copy(side, step):
        column = other_y if side == 0 else y
        return pltpu.make_async_copy(
            x_hbm.at[device_of(row_of(step), column, core)], x_ref.at[side, step],
            x_sems.at[side, step],
        )

    core_stats[core] = stats_ref[...]
    swapped = swap(core_stats, core_sems, core, partner)
    for side in range(2):
        for step in steps:
            core_copy(side, step).start()
    for side in range(2):
        for step in steps:
            x_copy(side, step).start()
    swapped.wait()
    chip_top, chip_total = combine(core_stats, CORES)
    y_stats[y, 0], y_stats[y, 1] = chip_top, chip_total
    across_stats = swap(y_stats, y_sems, y, across)
    for side in range(CORES):
        near[side] = jnp.exp(core_stats[side, 0] - chip_top)

    def down(row):
        return jnp.broadcast_to(row, (LANES, block_rows)).T

    def scaled(value, scale, target):
        spread = down(scale[pl.ds(target, 1), :])
        wide = value.astype(jnp.float32)
        return wide * jnp.concatenate([spread] * (wide.shape[1] // LANES), axis=1)

    def both(scales, side, step):
        target = device_of(row_of(step), other_y if side == 0 else y, core)
        x_copy(side, step).wait()
        core_copy(side, step).wait_recv()
        return scaled(x_ref[side, step], scales.at[core], target) + scaled(
            core_in[side, step], scales.at[other_core], target
        )

    for order, step in enumerate(steps):
        y_out[step] = both(near, 0, step).astype(y_out.dtype)
        y_copy(step).start()
        if order == 0:
            across_stats.wait()
            z_stats[z, 0], z_stats[z, 1] = combine(y_stats, 2)
            for other in range(1, rows_z):
                stats_copy(other, z).start()
    for step in range(1, rows_z):
        stats_copy(step, row_of(step)).wait_recv()
    top, total = combine(z_stats, rows_z)
    lse_ref[...] = top + jnp.log(total)
    totals[...] = total
    for side in range(CORES):
        factors[side] = jnp.exp(core_stats[side, 0] - top)
    factors[CORES] = jnp.exp(y_stats[other_y, 0] - top)
    for step in steps:
        total = both(factors, 1, step)
        y_copy(step).wait_recv()
        total = total + scaled(
            y_in[step], factors.at[CORES], device_of(row_of(step), y, core)
        )
        if step:
            z_out[step] = total.astype(z_out.dtype)
            z_copy(step).start()
    for step in range(1, rows_z):
        z_copy(step).wait_recv()
        total = total + z_in[step].astype(jnp.float32)
    over = down(totals[pl.ds(index, 1), :])
    total = total / jnp.concatenate([over] * (total.shape[1] // LANES), axis=1)
    width = total.shape[1]
    local_rows = out_ref.shape[0]
    for local in range(block_rows // local_rows):
        out_ref[:, local * width : (local + 1) * width] = total[
            local * local_rows : (local + 1) * local_rows
        ].astype(out_ref.dtype)
    for step in range(1, rows_z):
        stats_copy(step, z).wait_send()
    for step in steps:
        core_copy(0, step).wait_send()
        core_copy(1, step).wait_send()
        y_copy(step).wait_send()
        if step:
            z_copy(step).wait_send()


def reduce_partials(parts, stats, rows_z, query_rows):
    block = parts.shape[1:]
    vmem = pl.BlockSpec(memory_space=pltpu.VMEM)
    dma = pltpu.SemaphoreType.DMA
    width = block[0] // query_rows * block[1]
    return pl.pallas_call(
        functools.partial(reduce_kernel, rows_z),
        out_shape=(
            jax.ShapeDtypeStruct((query_rows, width), jnp.bfloat16),
            jax.ShapeDtypeStruct(stats.shape[1:], jnp.float32),
        ),
        in_specs=[pl.BlockSpec(memory_space=pl.ANY), vmem],
        out_specs=(vmem, vmem),
        scratch_shapes=[
            pltpu.VMEM((2, rows_z) + block, parts.dtype),
            dma((2, rows_z)),
            pltpu.VMEM((2, rows_z) + block, parts.dtype),
            pltpu.VMEM((rows_z,) + block, parts.dtype),
            pltpu.VMEM((rows_z,) + block, parts.dtype),
            pltpu.VMEM((rows_z,) + block, parts.dtype),
            pltpu.VMEM((rows_z,) + block, parts.dtype),
            pltpu.VMEM((CORES,) + stats.shape, jnp.float32),
            pltpu.VMEM((2,) + stats.shape, jnp.float32),
            pltpu.VMEM((rows_z,) + stats.shape, jnp.float32),
            pltpu.VMEM((CORES,) + stats.shape[1:], jnp.float32),
            pltpu.VMEM((CORES + 1,) + stats.shape[1:], jnp.float32),
            pltpu.VMEM(stats.shape[1:], jnp.float32),
            dma((2, rows_z)),
            dma((2, rows_z)),
            dma((rows_z,)),
            dma((rows_z,)),
            dma((rows_z,)),
            dma((rows_z,)),
            dma((2,)),
            dma((2,)),
            dma((rows_z,)),
            dma((rows_z,)),
        ],
        compiler_params=pltpu.CompilerParams(
            collective_id=2, has_side_effects=True, vmem_limit_bytes=vmem_limit
        ),
        name="reduce_partials",
    )(parts, stats)


def per_device(queries, cache, page_counts, slot_request, slot_start, slot_live, slot_pages):
    count = lax.axis_size("kv")
    requests, query_count, shard_width = queries.shape
    page_rows, token_width = cache.shape[1:]
    latent = token_width - ROPE
    heads = count * shard_width // token_width
    rows_z = count // (2 * CORES)
    slots = slot_request.shape[0]
    if shard_width % token_width or rows_z * 2 * CORES != count:
        return per_device_whole(
            queries, cache, page_counts, slot_request, slot_start, slot_live, slot_pages
        )
    local_heads = shard_width // token_width
    query_rows = query_count * requests
    shard = queries.transpose(1, 0, 2).reshape(query_rows, shard_width)
    page_ids = jnp.arange(cache.shape[0], dtype=jnp.int32)
    picks = (slot_pages.reshape(-1, 1) == page_ids[None, :]).astype(cache.dtype)
    gathered, keys = gather_queries(
        shard, picks, cache.transpose(1, 2, 0), slots, rows_z, query_count
    )
    parts, stats = attend_blocks(
        gathered, keys, page_counts, slot_request, slot_start, slot_live, count, query_count,
        page_rows, latent,
    )
    attended, lse = reduce_partials(parts, stats, rows_z, query_rows)
    attended = attended.reshape(query_count, requests, local_heads * latent).transpose(1, 0, 2)
    lse = lse.reshape(count * local_heads, query_count, requests).transpose(2, 1, 0)
    return (attended, lse)


def per_device_whole(queries, cache, page_counts, slot_request, slot_start, slot_live, slot_pages):
    count = lax.axis_size("kv")
    requests, query_count, shard_width = queries.shape
    token_width = cache.shape[2]
    latent = token_width - ROPE
    heads = count * shard_width // token_width
    rows = query_count * heads
    gathered = lax.all_gather(queries, "kv", axis=2, tiled=True)
    query_heads = gathered.reshape(requests, rows, token_width)
    numer, best, denom = attend_whole(
        query_heads, cache, page_counts, slot_request, slot_start, slot_live, slot_pages, latent,
        query_count,
    )
    best, denom = best[:, :, 0], denom[:, :, 0]
    highest = lax.pmax(best, "kv")
    total = lax.psum(denom * jnp.exp(best - highest), "kv")
    scaled = numer * jnp.exp(best - highest)[..., None]
    lse = (highest + jnp.log(total)).reshape(requests, query_count, heads)
    total = total.reshape(requests, query_count, heads)
    flat = lax.optimization_barrier(scaled.reshape(requests * query_count, heads * latent))
    width = heads * latent // count
    summed = lax.psum_scatter(flat, "kv", scatter_dimension=1, tiled=True)
    summed = summed.reshape(requests, query_count, width)
    first_head = lax.axis_index("kv") * width // latent
    picked_heads = max(1, width // latent)
    picked = lax.dynamic_slice_in_dim(total, first_head, picked_heads, 2)
    picked = jnp.repeat(picked, min(width, latent), axis=2)
    return ((summed / picked).astype(jnp.bfloat16), lse)


def solution(mesh):
    in_specs = (
        P("rep", None, "kv"),
        P(("rep", "kv"), None, None),
        P("rep"),
        P(("rep", "kv")),
        P(("rep", "kv")),
        P(("rep", "kv")),
        P(("rep", "kv"), None),
    )
    out_specs = (P("rep", None, "kv"), P("rep", None, None))
    return jax.shard_map(
        per_device, mesh=mesh, in_specs=in_specs, out_specs=out_specs, check_vma=False
    )
```
